32 devices in a mesh: row: 4 (over y, x), col: 8 (over z, core).
Axes of the slice: x: 2, y: 2, z: 4, core: 2. Of those that a mesh axis runs over, the one named last changes fastest.
Arguments:
- iterates: float32 [11, 1024], P(None, ('col', 'row')), may hold values from -6 to 6
- residuals: float32 [11, 1024], P(None, ('col', 'row')), may hold values from -3 to 3
- operator: float32 [16384, 1024], P('row', 'col'), may hold values from -0.1875 to 0.1875
- target: float32 [16384], replicated, may hold values from -6 to 6
- cone_id: int32 [16384], replicated, may hold values from 0 to 2047, never falling along the last dimension, each value on 1 to 16 neighbouring positions
Outputs:
- next_point: float32 [1024], P(('col', 'row'))
- projected: float32 [16384], P('row')
The draws below stay inside these ranges and needn't reach their ends.
Inputs may be any that keep to these rules, and one draw needn't show every extreme that they name: cone_id never falls along the rows; each of the 2048 cones holds 1 to 16 consecutive rows.
All inputs are finite; a program needn't handle non-finite values.
Results may differ from the reference program's by a relative error of at most 0.0003.
Values sent between devices are 32-bit elements; how exact they have to be, the bound alone decides.
No kernel may reach another device: no remote copies, remote signals or barrier semaphores. Data moves between devices by JAX's collectives and lax.ppermute only.
A program may use at most 64 MiB of HBM per device.

```python
import math
import jax
import jax.numpy as jnp
import numpy as np
from jax import lax

HIST = 10
N = 1024
M = 16384
NCONE = 2048
CMOST = 16


def level_of(key, dims, shards, low, largest):
    factor_of, own = 1.0, jax.random.fold_in(key, 6)
    for position, shards_of in shards:
        heights = jnp.exp(jax.random.uniform(jax.random.fold_in(own, position), (shards_of,), jnp.float32, low / len(shards), largest / len(shards)))
        factor_of = factor_of * jnp.repeat(heights, dims[position] // shards_of).reshape([-1 if axis == position else 1 for axis in range(len(dims))])
    return factor_of


def profile(amount, total, limit, skew):
    weights = [(1 << 20) // math.isqrt(standing ** skew) + 1 for standing in range(2, amount + 1)]
    spare, given = total - limit - (amount - 1), [1] * (amount - 1)
    while spare > 0:
        free = [i for i in range(amount - 1) if given[i] < limit]
        whole, left = sum([weights[i] for i in free]), spare
        for i in free:
            more = min(limit - given[i], max(1, left * weights[i] // whole), spare)
            given[i] = given[i] + more
            spare = spare - more
    return np.array([limit] + given)


def uneven_parts(own_key, count, total, limit, skew):
    if count == 2:
        one = jax.random.randint(own_key, (), max(1, total - limit), min(limit, total - 1) + 1)
        return jnp.stack([one, total - one])
    sizes = jnp.asarray(profile(count, total, limit, skew), jnp.int32)
    twos = (count - 1) // 2
    source_of, receiver = sizes[1:1 + 2 * twos:2], sizes[2:2 + 2 * twos:2]
    room = jnp.minimum(source_of - 1, limit - receiver)
    moved = jax.random.randint(jax.random.fold_in(own_key, 1), (twos,), 0, 1 << 20) % (room + 1)
    sizes = sizes.at[1:1 + 2 * twos:2].set(source_of - moved).at[2:2 + 2 * twos:2].set(receiver + moved)
    return sizes[jax.random.permutation(jax.random.fold_in(own_key, 2), count)]


def scatter_about(rng, shape, width, bound, cuts=(), held_as=jnp.bfloat16):
    drawn = jax.random.normal(rng, shape, jnp.float32) * width
    if len(cuts) > 0:
        drawn = level_of(rng, shape, cuts, -0.22, 0.18) * drawn
    return jnp.clip(drawn, min=-bound, max=bound).astype(held_as)


def setup_inputs(seed: int = 0) -> dict:
    key_of = jax.random.split(jax.random.key(seed), 6)
    return {
        "iterates": scatter_about(key_of[0], (HIST + 1, N), 1.0, 6.0, ((1, 32),), jnp.float32),
        "residuals": scatter_about(key_of[1], (HIST + 1, N), 0.5, 3.0, ((1, 32),), jnp.float32),
        "operator": scatter_about(key_of[2], (M, N), N ** -0.5, 0.1875, ((0, 4), (1, 8)), jnp.float32),
        "target": scatter_about(key_of[3], (M,), 1.0, 6.0, (), jnp.float32),
        "cone_id": jnp.searchsorted(jnp.cumsum(uneven_parts(key_of[4], NCONE, M, CMOST, 0)), jnp.arange(M), side="right").astype(jnp.int32),
    }


HIGH = lax.Precision.HIGHEST

def project_cones(slack, cone_id):
    head_mask = jnp.concatenate([jnp.ones((1,), slack.dtype), (cone_id[1:] != cone_id[:-1]).astype(slack.dtype)])
    head_tot = jax.ops.segment_sum(head_mask * slack, cone_id, num_segments=NCONE)
    tail_tot = jax.ops.segment_sum((1.0 - head_mask) * slack * slack, cone_id, num_segments=NCONE)
    head_row = head_tot[cone_id]
    norm_row = jnp.sqrt(tail_tot[cone_id])
    inside = norm_row <= head_row
    killed = norm_row <= -head_row
    safe_norm = jnp.where(norm_row > 0, norm_row, 1.0)
    middle = 0.5 * (head_row + norm_row)
    outside = jnp.where(head_mask > 0, middle, middle * slack / safe_norm)
    return jnp.where(inside, slack, jnp.where(killed, 0.0, outside))

def reference(iterates, residuals, operator, target, cone_id):
    delta_x = iterates[1:] - iterates[:-1]
    delta_f = residuals[1:] - residuals[:-1]
    last_f = residuals[-1]
    gram = jnp.dot(delta_f, delta_f.T, precision=HIGH)
    right_side = jnp.dot(delta_f, last_f, precision=HIGH)
    shifted = gram + 0.01 * (jnp.trace(gram) / HIST) * jnp.eye(HIST, dtype=gram.dtype)
    factor = jnp.linalg.cholesky(shifted)
    weights = jax.scipy.linalg.cho_solve((factor, True), right_side)
    blended = iterates[-1] + last_f - jnp.dot(weights, delta_x + delta_f, precision=HIGH)
    slack = target - jnp.dot(operator, blended, precision=HIGH)
    projected = project_cones(slack, cone_id)
    back = jnp.dot(projected - slack, operator, precision=HIGH)
    next_point = blended - math.sqrt(N / M) * back
    return (next_point, projected)
```

```python
import functools
import math

import jax
import jax.numpy as jnp
from jax import lax
from jax.experimental import pallas as pl
from jax.experimental.pallas import tpu as pltpu
from jax.sharding import PartitionSpec as P

RIM = 16
LANES = 128
TILE = 8
BF16 = jnp.bfloat16
F32 = jnp.float32
LIMIT = 24 * 1024 * 1024
SHIFTS = (1, 2, 4, 8)
NT = (((1,), (1,)), ((), ()))


def params(limit=LIMIT):
    return pltpu.CompilerParams(vmem_limit_bytes=limit)


def vmem():
    return pl.BlockSpec(memory_space=pltpu.VMEM)


def smem():
    return pl.BlockSpec(memory_space=pltpu.SMEM)


def tree(terms):
    terms = list(terms)
    while len(terms) > 1:
        terms = [a + b for a, b in zip(terms[::2], terms[1::2])]
    return terms[0]


def up(length):
    return -(-length // TILE) * TILE


def split(x):
    high = x.astype(BF16)
    return high, (x - high.astype(F32)).astype(BF16)


def shifted(x, step):
    rows, lanes = x.shape
    lane = lax.broadcasted_iota(jnp.int32, x.shape, 1)
    turned = pltpu.roll(x, step % lanes, 1)
    carried = pltpu.roll(turned, (1 if step > 0 else -1) % rows, 0)
    return jnp.where(lane < step if step > 0 else lane >= lanes + step, carried, turned)


def pack_kernel(hist, local, x_ref, f_ref, top_ref, low_ref, out_ref, dirs_ref, diff_ref):
    out_ref[...] = jnp.zeros_like(out_ref)
    dirs_ref[...] = jnp.zeros_like(dirs_ref)
    diff_ref[...] = jnp.zeros_like(diff_ref)
    delta_f = f_ref[1 : hist + 1, :] - f_ref[0:hist, :]
    delta_x = x_ref[1 : hist + 1, :] - x_ref[0:hist, :]
    last_f = f_ref[hist : hist + 1, :]
    diff_ref[0:hist, :] = delta_f
    diff_ref[hist : hist + 1, :] = last_f
    dirs_ref[0:hist, :] = delta_x + delta_f
    dirs_ref[hist : hist + 1, :] = x_ref[hist : hist + 1, :] + last_f
    diff = diff_ref[...]
    gram = lax.dot_general(diff, diff, NT, precision=lax.Precision.HIGHEST, preferred_element_type=F32)
    wide = gram.shape[0]
    out_ref[0:wide, 0:local] = dirs_ref[...]
    out_ref[0:wide, local : local + wide] = gram
    out_ref[wide : wide + RIM, 0 : top_ref.shape[1]] = top_ref[...]
    out_ref[wide + RIM : wide + 2 * RIM, 0 : low_ref.shape[1]] = low_ref[...]


def image_kernel(hist, local, row_count, chunk, row_ref, *refs):
    parts = refs[:row_count]
    oper_ref, target_ref, ids_ref, cat_ref, img_ref, dirs_ref, aux_ref = refs[row_count:]
    row = row_ref[0]
    row_block, width = oper_ref.shape
    wide = up(hist + 1)
    wide = -(-wide // 16) * 16
    own_rows = row_block // LANES
    ext_rows = own_rows + TILE

    lane = lax.broadcasted_iota(jnp.int32, (wide, width), 1)
    dirs = jnp.zeros((wide, width), F32)
    for turn in range(row_count):
        place = lax.bitwise_xor(row, turn)
        block = parts[turn][0:wide, 0:LANES]
        if width > LANES:
            block = jnp.concatenate([block] * (width // LANES), axis=1)
        for slot in range(row_count):
            moved = pltpu.roll(block, slot * local, 1) if slot else block
            dirs = jnp.where((lane // local == slot) & (place == slot), moved, dirs)
    dirs_ref[...] = dirs
    high, low = split(dirs)
    left = jnp.concatenate(
        [jnp.concatenate([high, high], axis=1), jnp.concatenate([low, jnp.zeros_like(low)], axis=1)], axis=0
    )

    def multiply(tile):
        both = lax.dot_general(left, tile, NT, preferred_element_type=F32)
        return both[0:wide, :] + both[wide : 2 * wide, :]

    for start in range(0, row_block, chunk):
        high, low = split(oper_ref[start : start + chunk, :])
        cat_ref[start : start + chunk, 0:width] = high
        cat_ref[start : start + chunk, width : 2 * width] = low
        image = multiply(jnp.concatenate([high, low], axis=1))
        for piece in range(chunk // LANES):
            tile = image[:, piece * LANES : (piece + 1) * LANES]
            img_ref[pl.ds(start // LANES + piece, hist + 1, stride=ext_rows), :] = tile[0 : hist + 1, :]

    after = jnp.zeros((RIM, width), F32)
    before = jnp.zeros((RIM, width), F32)
    for turn in range(row_count):
        place = lax.bitwise_xor(row, turn)
        after = jnp.where(place == row + 1, parts[turn][wide : wide + RIM, 0:width], after)
        before = jnp.where(place == row - 1, parts[turn][wide + RIM : wide + 2 * RIM, 0:width], before)
    edge = jnp.concatenate([after, jnp.zeros((LANES - 2 * RIM, width), F32), before], axis=0)
    high, low = split(edge)
    tile = multiply(jnp.concatenate([high, low], axis=1))
    for place in range(own_rows, ext_rows):
        img_ref[pl.ds(place, hist + 1, stride=ext_rows), :] = tile[0 : hist + 1, :]

    last = ids_ref.shape[0] - 1
    first = row * own_rows
    follow = jnp.minimum(first + own_rows, last)
    ahead = jnp.maximum(first - 1, 0)
    lane1 = lax.broadcasted_iota(jnp.int32, (1, LANES), 1)
    has_next = (first + own_rows) <= last
    ids_next = jnp.where((lane1 < RIM) & has_next, ids_ref[pl.ds(follow, 1), :], -1)
    ids_prev = jnp.where((lane1 >= LANES - RIM) & (first > 0), ids_ref[pl.ds(ahead, 1), :], -1)
    ids = jnp.concatenate(
        [ids_ref[pl.ds(first, own_rows), :], ids_next, jnp.full((TILE - 2, LANES), -1, jnp.int32), ids_prev], axis=0
    )
    aux_ref[0] = jnp.concatenate(
        [
            target_ref[pl.ds(first, own_rows), :],
            target_ref[pl.ds(follow, 1), :],
            jnp.zeros((TILE - 2, LANES), F32),
            target_ref[pl.ds(ahead, 1), :],
        ],
        axis=0,
    )
    for index, step in enumerate(SHIFTS):
        same = (shifted(ids, step) == ids).astype(F32)
        aux_ref[2 + index] = same
        aux_ref[2 + len(SHIFTS) + index] = (shifted(ids, -step) == ids).astype(F32)
        if step == 1:
            aux_ref[1] = 1.0 - same


def solve_kernel(hist, local, count, *refs):
    grams = refs[:count]
    img_ref, dirs_ref, part_ref, blend_ref = refs[count:]
    wide, width = dirs_ref.shape
    gram = tree(g[...] for g in grams)
    index = lax.broadcasted_iota(jnp.int32, (wide, LANES), 0)
    cols = [jnp.broadcast_to(gram[:, local + j : local + j + 1], (wide, LANES)) for j in range(hist + 1)]

    def row_of(x, k):
        return jnp.broadcast_to(x[k : k + 1, :], (wide, LANES))

    trace = row_of(cols[0], 0)
    for k in range(1, hist):
        trace = trace + row_of(cols[k], k)
    ridge = 0.01 * (trace / hist)
    for k in range(hist):
        cols[k] = jnp.where(index == k, cols[k] + ridge, cols[k])
    for k in range(hist):
        inverse = 1.0 / row_of(cols[k], k)
        for j in range(k + 1, hist + 1):
            ratio = row_of(cols[j], k) * inverse
            cols[j] = jnp.where(index == k, ratio, cols[j] - cols[k] * ratio)
    weights = cols[hist]

    ext_rows = part_ref.shape[0]
    total = img_ref[hist * ext_rows : (hist + 1) * ext_rows, :]
    for k in range(hist):
        total = total - jnp.broadcast_to(weights[k : k + 1, :], (ext_rows, LANES)) * img_ref[k * ext_rows : (k + 1) * ext_rows, :]
    part_ref[...] = total
    factors = jnp.where(index < hist, -weights, jnp.where(index == hist, 1.0, 0.0))
    for start in range(0, width, LANES):
        blend_ref[:, start : start + LANES] = jnp.sum(factors * dirs_ref[:, start : start + LANES], axis=0, keepdims=True)


def cone_kernel(count, *refs):
    parts = refs[:count]
    aux_ref, cat_ref, proj_ref, back_ref = refs[count:]
    slack = aux_ref[0] - tree(p[...] for p in parts)
    head = aux_ref[1]
    square = (1.0 - head) * slack * slack
    lead, ahead, behind = head * slack, square, square
    for index, step in enumerate(SHIFTS):
        same = aux_ref[2 + index]
        lead = lead + same * shifted(lead, step)
        ahead = ahead + same * shifted(ahead, step)
        behind = behind + aux_ref[2 + len(SHIFTS) + index] * shifted(behind, -step)
    norm = jnp.sqrt(jnp.maximum(ahead + behind - square, 0.0))
    inside = norm <= lead
    killed = norm <= -lead
    safe = jnp.where(norm > 0, norm, 1.0)
    middle = 0.5 * (lead + norm)
    outside = jnp.where(head > 0, middle, middle * slack / safe)
    projected = jnp.where(inside, slack, jnp.where(killed, 0.0, outside))
    own_rows = proj_ref.shape[0]
    proj_ref[...] = projected[0:own_rows, :]
    correction = projected[0:own_rows, :] - slack[0:own_rows, :]
    high, low = split(correction)
    high, low = high.astype(F32), low.astype(F32)
    sub = lax.broadcasted_iota(jnp.int32, (TILE, LANES), 0)
    pieces = []
    for piece in range(own_rows):
        base = piece // TILE * TILE
        mine = sub == piece % TILE
        pieces.append(
            jnp.concatenate(
                [jnp.where(mine, high[base : base + TILE, :], 0.0), jnp.where(mine, low[base : base + TILE, :], 0.0)], axis=0
            ).astype(BF16)
        )
    left = jnp.concatenate(pieces, axis=1)
    both = jnp.dot(left, cat_ref[...], preferred_element_type=F32)
    width = back_ref.shape[1]
    sums = both[0:TILE, 0:width] + both[0:TILE, width : 2 * width] + both[TILE : 2 * TILE, 0:width]
    back_ref[...] = jnp.sum(sums, axis=0, keepdims=True)


def xor_pairs(count, turn):
    return [(i, i ^ turn) for i in range(count)]


def exchange(x, axis, turns):
    count = lax.axis_size(axis)
    return [lax.ppermute(x, axis, xor_pairs(count, turn)) for turn in turns]


def col_stages(count):
    stages, bit = [[1]], 2
    while bit < count:
        stages.append([bit, 2 * bit, 3 * bit] if 2 * bit < count else [bit])
        bit *= 4
    return stages


def reduce_col(x, count):
    stages = col_stages(count)
    for turns in stages[:-1]:
        x = tree([x, *exchange(x, "col", turns)])
    return [x, *exchange(x, "col", stages[-1])]


def body(iterates, residuals, operator, target, cone_id):
    row_count = lax.axis_size("row")
    col_count = lax.axis_size("col")
    row_block, width = operator.shape
    hist, local = iterates.shape[0] - 1, iterates.shape[1]
    all_rows = row_block * row_count
    scale_back = math.sqrt(local * row_count * col_count / all_rows)
    wide = -(-(hist + 1) // 16) * 16
    own_rows = row_block // LANES
    ext_rows = own_rows + TILE
    row = lax.axis_index("row")
    row_arg = row.astype(jnp.int32).reshape(1)

    message = pl.pallas_call(
        functools.partial(pack_kernel, hist, local),
        name="pack",
        grid=(1,),
        in_specs=[
            pl.BlockSpec((hist + 1, local), lambda i: (0, 0)),
            pl.BlockSpec((hist + 1, local), lambda i: (0, 0)),
            pl.BlockSpec((RIM, width), lambda i: (0, 0)),
            pl.BlockSpec((RIM, width), lambda i: (row_block // RIM - 1, 0)),
        ],
        out_specs=pl.BlockSpec((wide + 2 * RIM, width), lambda i: (0, 0)),
        out_shape=jax.ShapeDtypeStruct((wide + 2 * RIM, width), F32),
        scratch_shapes=[pltpu.VMEM((wide, local), F32), pltpu.VMEM((wide, local), F32)],
        compiler_params=params(),
    )(iterates, residuals, operator, operator)
    messages = [message, *exchange(message, "row", range(1, row_count))]

    gram = tree(m[0:wide, 0:LANES] for m in messages)
    grams = reduce_col(gram, col_count)

    cat, img, dirs, aux = pl.pallas_call(
        functools.partial(image_kernel, hist, local, row_count, min(512, row_block)),
        name="image",
        in_specs=[smem()] + [vmem()] * (row_count + 3),
        out_specs=[vmem()] * 4,
        out_shape=[
            jax.ShapeDtypeStruct((row_block, 2 * width), BF16),
            jax.ShapeDtypeStruct(((hist + 1) * ext_rows, LANES), F32),
            jax.ShapeDtypeStruct((wide, width), F32),
            jax.ShapeDtypeStruct((2 + 2 * len(SHIFTS), ext_rows, LANES), F32),
        ],
        compiler_params=params(),
    )(row_arg, *messages, operator, target.reshape(-1, LANES), cone_id.reshape(-1, LANES))

    part, blended = pl.pallas_call(
        functools.partial(solve_kernel, hist, local, len(grams)),
        name="solve",
        in_specs=[vmem()] * (len(grams) + 2),
        out_specs=[vmem()] * 2,
        out_shape=[jax.ShapeDtypeStruct((ext_rows, LANES), F32), jax.ShapeDtypeStruct((1, width), F32)],
        compiler_params=params(),
    )(*grams, img, dirs)

    parts = reduce_col(part, col_count)
    projected, back = pl.pallas_call(
        functools.partial(cone_kernel, len(parts)),
        name="cones",
        in_specs=[vmem()] * (len(parts) + 2),
        out_specs=[vmem()] * 2,
        out_shape=[jax.ShapeDtypeStruct((own_rows, LANES), F32), jax.ShapeDtypeStruct((1, width), F32)],
        compiler_params=params(),
    )(*parts, aux, cat)

    back = tree([back, *exchange(back, "row", range(1, row_count))])
    moved = blended - scale_back * back
    next_point = lax.dynamic_slice_in_dim(moved, row * local, local, 1)
    return (next_point.reshape(local), projected.reshape(row_block))


def solution(mesh):
    return jax.shard_map(
        body,
        mesh=mesh,
        in_specs=(P(None, ("col", "row")), P(None, ("col", "row")), P("row", "col"), P(), P()),
        out_specs=(P(("col", "row")), P("row")),
        check_vma=False,
    )
```

```python
import functools
import math

import jax
import jax.numpy as jnp
from jax import lax
from jax.experimental import pallas as pl
from jax.experimental.pallas import tpu as pltpu
from jax.sharding import PartitionSpec as P

LANES = 128
TILE = 8
BF16 = jnp.bfloat16
F32 = jnp.float32
LIMIT = 24 * 1024 * 1024
SHIFTS = (1, 2, 4, 8)
NT = (((1,), (1,)), ((), ()))
TARGET, HEAD, FIRST, LAST, UPWARD, DOWNWARD = 0, 1, 2, 3, 4, 4 + len(SHIFTS)
AUX = 4 + 2 * len(SHIFTS)
BACK, TAIL_LAST, HEAD_LAST, TAIL_FIRST, SQUARE_LAST, LEAD_LAST, SQUARE_FIRST = range(7)


def params():
    return pltpu.CompilerParams(vmem_limit_bytes=LIMIT)


def vmem():
    return pl.BlockSpec(memory_space=pltpu.VMEM)


def smem():
    return pl.BlockSpec(memory_space=pltpu.SMEM)


def hbm(x):
    return pltpu.with_memory_space_constraint(x, pltpu.HBM)


def tree(terms):
    terms = list(terms)
    while len(terms) > 1:
        terms = [a + b for a, b in zip(terms[::2], terms[1::2])]
    return terms[0]


def split(x):
    high = x.astype(BF16)
    return high, (x - high.astype(F32)).astype(BF16)


def shifted(x, step):
    rows, lanes = x.shape
    lane = lax.broadcasted_iota(jnp.int32, x.shape, 1)
    turned = pltpu.roll(x, step % lanes, 1)
    carried = pltpu.roll(turned, (1 if step > 0 else -1) % rows, 0)
    return jnp.where(lane < step if step > 0 else lane >= lanes + step, carried, turned)


def dims(hist, local):
    wide = -(-(hist + 1) // 16) * 16
    return wide, LANES // local, wide * local // LANES


def pack_kernel(hist, local, x_any, f_any, out_ref, x_ref, f_ref, dirs_ref, diff_ref, sems):
    wide, group, rows = dims(hist, local)
    copies = [pltpu.make_async_copy(a, b, sems.at[i]) for i, (a, b) in enumerate(((x_any, x_ref), (f_any, f_ref)))]
    for copy in copies:
        copy.start()
    dirs_ref[...] = jnp.zeros_like(dirs_ref)
    diff_ref[...] = jnp.zeros_like(diff_ref)
    for copy in copies:
        copy.wait()
    delta_f = f_ref[1 : hist + 1, :] - f_ref[0:hist, :]
    delta_x = x_ref[1 : hist + 1, :] - x_ref[0:hist, :]
    last_f = f_ref[hist : hist + 1, :]
    diff_ref[0:hist, :] = delta_f
    diff_ref[hist : hist + 1, :] = last_f
    dirs_ref[0:hist, 0:local] = delta_x + delta_f
    dirs_ref[hist : hist + 1, 0:local] = x_ref[hist : hist + 1, :] + last_f
    gram = lax.dot_general(diff_ref[0:wide, :], diff_ref[...], NT, precision=lax.Precision.HIGHEST, preferred_element_type=F32)
    sub = lax.broadcasted_iota(jnp.int32, gram.shape, 0)
    gram = jnp.where(sub < hist, gram, 0.0)
    flat = jnp.zeros((TILE, LANES), F32)
    for start in range(0, wide, TILE):
        turned = pltpu.roll(gram[start : start + TILE, :], 0, 1, stride=hist + 1, stride_axis=0)
        flat = flat + (pltpu.roll(turned, start * (hist + 1) % LANES, 1) if start else turned)
    message = dirs_ref[pl.ds(0, rows, stride=group), :]
    for place in range(1, group):
        message = message + pltpu.roll(dirs_ref[pl.ds(place, rows, stride=group), :], place * local, 1)
    sub = lax.broadcasted_iota(jnp.int32, message.shape, 0)
    message = jnp.where(sub == rows - 1, jnp.sum(flat, axis=0, keepdims=True), message)
    message = jnp.concatenate([message] * (TILE // rows), axis=0)
    for start in range(0, out_ref.shape[0], TILE):
        out_ref[start : start + TILE, :] = message


def split_kernel(message_any, oper_ref, cat_ref):
    width = oper_ref.shape[1]
    high, low = split(oper_ref[...])
    cat_ref[:, 0:width] = high
    cat_ref[:, width : 2 * width] = low


def image_kernel(hist, local, row_count, chunk, where_ref, recv_ref, cat_ref, part_ref, blend_ref, dirs_ref, img_ref):
    wide, group, rows = dims(hist, local)
    row_block, width = cat_ref.shape[0], cat_ref.shape[1] // 2
    own_rows = row_block // LANES
    mine = recv_ref[pl.ds(pl.multiple_of(where_ref[1] * (row_count * rows), TILE), row_count * rows), :]
    lane = lax.broadcasted_iota(jnp.int32, (rows, LANES), 1)
    for start in range(0, width, LANES):
        for place in range(group):
            spread = jnp.zeros((rows, LANES), F32)
            for slot in range(group):
                block = start // local + slot
                moved = mine[block * rows : (block + 1) * rows, :]
                if slot != place:
                    moved = pltpu.roll(moved, (slot - place) * local % LANES, 1)
                spread = jnp.where(lane // local == slot, moved, spread)
            dirs_ref.at[start // LANES][pl.ds(place, rows, stride=group), :] = spread
    sub = lax.broadcasted_iota(jnp.int32, (wide, width), 0)
    dirs = jnp.concatenate([dirs_ref[i] for i in range(width // LANES)], axis=1)
    dirs = jnp.where(sub <= hist, dirs, 0.0)
    high, low = split(dirs)
    left = jnp.concatenate(
        [jnp.concatenate([high, high], axis=1), jnp.concatenate([low, jnp.zeros_like(low)], axis=1)], axis=0
    )
    for start in range(0, row_block, chunk):
        both = lax.dot_general(left, cat_ref[start : start + chunk, :], NT, preferred_element_type=F32)
        image = both[0:wide, :] + both[wide : 2 * wide, :]
        for piece in range(chunk // LANES):
            tile = image[:, piece * LANES : (piece + 1) * LANES]
            img_ref[pl.ds(start // LANES + piece, hist + 1, stride=own_rows), :] = tile[0 : hist + 1, :]

    flat = jnp.sum(recv_ref[pl.ds(rows - 1, recv_ref.shape[0] // rows, stride=rows), :], axis=0, keepdims=True)
    index = lax.broadcasted_iota(jnp.int32, (wide, LANES), 0)
    gram = jnp.where(index == 0, flat, 0.0)
    for k in range(1, hist):
        gram = jnp.where(index == k, pltpu.roll(flat, LANES - k * (hist + 1), 1), gram)
    cols = [jnp.broadcast_to(gram[:, j : j + 1], (wide, LANES)) for j in range(hist + 1)]

    def row_of(x, k):
        return jnp.broadcast_to(x[k : k + 1, :], (wide, LANES))

    trace = row_of(cols[0], 0)
    for k in range(1, hist):
        trace = trace + row_of(cols[k], k)
    ridge = 0.01 * (trace / hist)
    for k in range(hist):
        cols[k] = jnp.where(index == k, cols[k] + ridge, cols[k])
    for k in range(hist):
        inverse = 1.0 / row_of(cols[k], k)
        for j in range(k + 1, hist + 1):
            ratio = row_of(cols[j], k) * inverse
            cols[j] = jnp.where(index == k, ratio, cols[j] - cols[k] * ratio)
    weights = cols[hist]
    total = img_ref[hist * own_rows : (hist + 1) * own_rows, :]
    for k in range(hist):
        total = total - jnp.broadcast_to(weights[k : k + 1, :], (own_rows, LANES)) * img_ref[k * own_rows : (k + 1) * own_rows, :]
    part_ref[...] = total
    factors = jnp.where(index < hist, -weights, jnp.where(index == hist, 1.0, 0.0))
    for start in range(0, width, LANES):
        blend_ref[:, start : start + LANES] = jnp.sum(factors * dirs[:, start : start + LANES], axis=0, keepdims=True)


def mask_kernel(row_count, where_ref, ids_ref, target_ref, blend_ref, aux_ref):
    own_rows = aux_ref.shape[1]
    row = where_ref[0]
    first = row * own_rows
    ids = ids_ref[pl.ds(first, own_rows), :]
    before = ids_ref[pl.ds(jnp.maximum(first - 1, 0), 1), :]
    after = ids_ref[pl.ds(jnp.minimum(first + own_rows, ids_ref.shape[0] - 1), 1), :]
    before = jnp.broadcast_to(before[:, LANES - 1 :], (1, LANES))
    after = jnp.broadcast_to(after[:, 0:1], (1, LANES))
    opens = ((ids == before) & (row > 0)).astype(F32)
    aux_ref[TARGET] = target_ref[pl.ds(first, own_rows), :]
    aux_ref[FIRST] = opens
    aux_ref[LAST] = ((ids == after) & (row < row_count - 1)).astype(F32)
    for index, step in enumerate(SHIFTS):
        same = (shifted(ids, step) == ids).astype(F32)
        aux_ref[UPWARD + index] = same
        aux_ref[DOWNWARD + index] = (shifted(ids, -step) == ids).astype(F32)
        if step == 1:
            aux_ref[HEAD] = (1.0 - same) * (1.0 - opens)


def cone_kernel(count, *refs):
    parts = refs[:count]
    aux_ref, cat_ref, proj_ref, edge_ref, out_ref = refs[count:]
    own_rows = proj_ref.shape[0]
    width = out_ref.shape[1]
    slack = aux_ref[TARGET] - tree(p[...] for p in parts)
    head, first, last = aux_ref[HEAD], aux_ref[FIRST], aux_ref[LAST]
    square = (1.0 - head) * slack * slack
    lead, ahead, behind = head * slack, square, square
    for index, step in enumerate(SHIFTS):
        same = aux_ref[UPWARD + index]
        lead = lead + same * shifted(lead, step)
        ahead = ahead + same * shifted(ahead, step)
        behind = behind + aux_ref[DOWNWARD + index] * shifted(behind, -step)
    norm = jnp.sqrt(jnp.maximum(ahead + behind - square, 0.0))
    inside = norm <= lead
    killed = norm <= -lead
    safe = jnp.where(norm > 0, norm, 1.0)
    middle = 0.5 * (lead + norm)
    outside = jnp.where(head > 0, middle, middle * slack / safe)
    projected = jnp.where(inside, slack, jnp.where(killed, 0.0, outside))
    proj_ref[...] = projected
    correction = jnp.where(first + last > 0, 0.0, projected - slack)

    sub = lax.broadcasted_iota(jnp.int32, (TILE, LANES), 0)
    final = own_rows - 1
    begin = (first * slack)[0:1, :]
    tail = (last * (1.0 - head) * slack)[final:, :]
    lead = (last * head)[final:, :]
    closing = jnp.where(sub == TAIL_LAST, tail, jnp.where(sub == HEAD_LAST, lead, 0.0))
    opening = jnp.where(sub == TAIL_FIRST, begin, 0.0)
    pieces = []
    for piece in range(own_rows):
        base = piece // TILE * TILE
        interior = jnp.where(sub == piece % TILE, correction[base : base + TILE, :], 0.0)
        edge = opening if piece == 0 else closing if piece == final else jnp.zeros_like(opening)
        high = jnp.concatenate([interior, edge], axis=0).astype(BF16)
        low = (jnp.concatenate([interior, edge], axis=0) - high.astype(F32)).astype(BF16)
        pieces.append(jnp.concatenate([high, low], axis=0))
    left = jnp.concatenate(pieces, axis=1)
    both = jnp.dot(left, cat_ref[...], preferred_element_type=F32)
    half = 2 * TILE
    sums = both[0:half, 0:width] + both[0:half, width : 2 * width] + both[half : 2 * half, 0:width]
    ends = slack[final:, :]
    scalars = jnp.where(
        sub == SQUARE_LAST,
        tail * ends,
        jnp.where(sub == LEAD_LAST, lead * ends, jnp.where(sub == SQUARE_FIRST, begin * slack[0:1, :], 0.0)),
    )
    scalars = jnp.broadcast_to(jnp.sum(scalars, axis=1, keepdims=True), (TILE, width))
    wide_sub = lax.broadcasted_iota(jnp.int32, (TILE, width), 0)
    out_ref[...] = jnp.where(
        wide_sub == BACK,
        jnp.sum(sums[0:TILE, :], axis=0, keepdims=True),
        jnp.where(wide_sub <= TAIL_FIRST, sums[TILE:half, :], scalars),
    )
    edge_ref[...] = jnp.where(sub == 0, slack[0:1, :], ends)


def finish_kernel(scale_back, local, row_count, where_ref, *refs):
    messages = refs[:row_count]
    proj_ref, edge_ref, aux_ref, blend_ref, next_ref, out_ref = refs[row_count:]
    row = where_ref[0]
    own_rows, width = proj_ref.shape[0], blend_ref.shape[1]
    received = [m[...] for m in messages]
    blocks = []
    for block in range(row_count):
        mine = received[0]
        for turn in range(1, row_count):
            mine = jnp.where(lax.bitwise_xor(row, turn) == block, received[turn], mine)
        blocks.append(mine)
    total = tree(b[BACK : BACK + 1, :] for b in blocks)
    ones = jnp.ones((1, LANES), F32)
    zeros = jnp.zeros((1, LANES), F32)
    tail_last, lead_last, tail_first = ones, zeros, ones
    for block in range(row_count - 1):
        this, that = blocks[block], blocks[block + 1]
        lead = this[LEAD_LAST : LEAD_LAST + 1, :]
        norm = jnp.sqrt(this[SQUARE_LAST : SQUARE_LAST + 1, :] + that[SQUARE_FIRST : SQUARE_FIRST + 1, :])
        inside = norm <= lead
        killed = norm <= -lead
        safe = jnp.where(norm > 0, norm, 1.0)
        middle = 0.5 * (lead + norm)
        factor = jnp.where(inside, 1.0, jnp.where(killed, 0.0, middle / safe))
        new = jnp.where(inside, lead, jnp.where(killed, 0.0, middle))
        tails = this[TAIL_LAST : TAIL_LAST + 1, :] + that[TAIL_FIRST : TAIL_FIRST + 1, :]
        total = total + ((factor - 1.0) * tails + (new - lead) * this[HEAD_LAST : HEAD_LAST + 1, :])
        tail_last = jnp.where(row == block, factor[:, 0:LANES], tail_last)
        lead_last = jnp.where(row == block, new[:, 0:LANES], lead_last)
        tail_first = jnp.where(row == block + 1, factor[:, 0:LANES], tail_first)
    moved = blend_ref[...] - scale_back * total
    mine = moved[:, 0:local]
    for block in range(1, row_count):
        mine = jnp.where(row == block, moved[:, block * local : (block + 1) * local], mine)
    next_ref[...] = mine
    final = own_rows - 1
    begin, end = edge_ref[0:1, :], edge_ref[1:2, :]
    ahead = jnp.where(aux_ref[FIRST, 0:1, :] > 0, tail_first * begin, proj_ref[0:1, :])
    closing = jnp.where(aux_ref[HEAD, final : final + 1, :] > 0, lead_last, tail_last * end)
    closing = jnp.where(aux_ref[LAST, final : final + 1, :] > 0, closing, proj_ref[final : final + 1, :])
    sub = lax.broadcasted_iota(jnp.int32, (own_rows, LANES), 0)
    out_ref[...] = jnp.where(sub == 0, ahead, jnp.where(sub == final, closing, proj_ref[...]))


def exchange(x, axis, turns):
    count = lax.axis_size(axis)
    return [lax.ppermute(x, axis, [(i, i ^ turn) for i in range(count)]) for turn in turns]


def reduce_col(x, count):
    stages, bit = [[1]], 2
    while bit < count:
        stages.append([bit, 2 * bit, 3 * bit] if 2 * bit < count else [bit])
        bit *= 4
    for turns in stages[:-1]:
        x = tree([x, *exchange(x, "col", turns)])
    return [x, *exchange(x, "col", stages[-1])]


def body(iterates, residuals, operator, target, cone_id):
    row_count = lax.axis_size("row")
    col_count = lax.axis_size("col")
    row_block, width = operator.shape
    hist, local = iterates.shape[0] - 1, iterates.shape[1]
    all_rows = row_block * row_count
    scale_back = math.sqrt(local * row_count * col_count / all_rows)
    wide, _, rows = dims(hist, local)
    own_rows = row_block // LANES
    where = jnp.stack([lax.axis_index("row"), lax.axis_index("col")]).astype(jnp.int32)

    message = pl.pallas_call(
        functools.partial(pack_kernel, hist, local),
        name="pack",
        in_specs=[pl.BlockSpec(memory_space=pltpu.HBM)] * 2,
        out_specs=vmem(),
        out_shape=jax.ShapeDtypeStruct((row_count * col_count * rows, LANES), F32),
        scratch_shapes=[
            pltpu.VMEM((hist + 1, local), F32),
            pltpu.VMEM((hist + 1, local), F32),
            pltpu.VMEM((wide, LANES), F32),
            pltpu.VMEM((LANES, local), F32),
            pltpu.SemaphoreType.DMA((2,)),
        ],
        compiler_params=params(),
    )(hbm(iterates), hbm(residuals))
    received = lax.all_to_all(message, ("col", "row"), 0, 0, tiled=True)

    step = min(512, row_block)
    cat = pl.pallas_call(
        split_kernel,
        name="split",
        grid=(row_block // step,),
        in_specs=[pl.BlockSpec(memory_space=pl.ANY), pl.BlockSpec((step, width), lambda i: (i, 0))],
        out_specs=pl.BlockSpec((step, 2 * width), lambda i: (i, 0)),
        out_shape=jax.ShapeDtypeStruct((row_block, 2 * width), BF16),
        compiler_params=params(),
    )(message, hbm(operator))

    part, blended = pl.pallas_call(
        functools.partial(image_kernel, hist, local, row_count, step),
        name="image",
        in_specs=[smem(), vmem(), vmem()],
        out_specs=[vmem()] * 2,
        out_shape=[
            jax.ShapeDtypeStruct((own_rows, LANES), F32),
            jax.ShapeDtypeStruct((1, width), F32),
        ],
        scratch_shapes=[pltpu.VMEM((width // LANES, wide, LANES), F32), pltpu.VMEM(((hist + 1) * own_rows, LANES), F32)],
        compiler_params=params(),
    )(where, received, cat)

    aux = pl.pallas_call(
        functools.partial(mask_kernel, row_count),
        name="masks",
        in_specs=[smem(), vmem(), vmem(), vmem()],
        out_specs=vmem(),
        out_shape=jax.ShapeDtypeStruct((AUX, own_rows, LANES), F32),
        compiler_params=params(),
    )(where, cone_id.reshape(-1, LANES), target.reshape(-1, LANES), blended)

    parts = reduce_col(part, col_count)
    projected, edge, back = pl.pallas_call(
        functools.partial(cone_kernel, len(parts)),
        name="cones",
        in_specs=[vmem()] * (len(parts) + 2),
        out_specs=[vmem()] * 3,
        out_shape=[
            jax.ShapeDtypeStruct((own_rows, LANES), F32),
            jax.ShapeDtypeStruct((TILE, LANES), F32),
            jax.ShapeDtypeStruct((TILE, width), F32),
        ],
        compiler_params=params(),
    )(*parts, aux, cat)

    next_point, projected = pl.pallas_call(
        functools.partial(finish_kernel, scale_back, local, row_count),
        name="finish",
        in_specs=[smem()] + [vmem()] * (row_count + 4),
        out_specs=[vmem()] * 2,
        out_shape=[jax.ShapeDtypeStruct((1, local), F32), jax.ShapeDtypeStruct((own_rows, LANES), F32)],
        compiler_params=params(),
    )(where, back, *exchange(back, "row", range(1, row_count)), projected, edge, aux, blended)
    return (next_point.reshape(local), projected.reshape(row_block))


def solution(mesh):
    return jax.shard_map(
        body,
        mesh=mesh,
        in_specs=(P(None, ("col", "row")), P(None, ("col", "row")), P("row", "col"), P(), P()),
        out_specs=(P(("col", "row")), P("row")),
        check_vma=False,
    )
```

```python
import functools
import math

import jax
import jax.numpy as jnp
from jax import lax
from jax.experimental import pallas as pl
from jax.experimental.pallas import tpu as pltpu
from jax.sharding import PartitionSpec as P

LANES = 128
TILE = 8
BF16 = jnp.bfloat16
F32 = jnp.float32
LIMIT = 24 * 1024 * 1024
SHIFTS = (1, 2, 4, 8)
NT = (((1,), (1,)), ((), ()))
TARGET, HEAD, FIRST, LAST, UPWARD, DOWNWARD = 0, 1, 2, 3, 4, 4 + len(SHIFTS)
AUX = 4 + 2 * len(SHIFTS)
BACK, TAIL_LAST, HEAD_LAST, TAIL_FIRST, SQUARE_LAST, LEAD_LAST, SQUARE_FIRST = range(7)


def params():
    return pltpu.CompilerParams(vmem_limit_bytes=LIMIT)


def vmem():
    return pl.BlockSpec(memory_space=pltpu.VMEM)


def hbm(x):
    return pltpu.with_memory_space_constraint(x, pltpu.HBM)


def tree(terms):
    terms = list(terms)
    while len(terms) > 1:
        terms = [a + b for a, b in zip(terms[::2], terms[1::2])]
    return terms[0]


def split(x):
    high = x.astype(BF16)
    return high, (x - high.astype(F32)).astype(BF16)


def shifted(x, step):
    rows, lanes = x.shape
    lane = lax.broadcasted_iota(jnp.int32, x.shape, 1)
    turned = pltpu.roll(x, step % lanes, 1)
    carried = pltpu.roll(turned, (1 if step > 0 else -1) % rows, 0)
    return jnp.where(lane < step if step > 0 else lane >= lanes + step, carried, turned)


def dims(hist, local):
    wide = -(-(hist + 1) // 16) * 16
    return wide, LANES // local, wide * local // LANES


def pack_kernel(hist, local, x_any, f_any, out_ref, x_ref, f_ref, dirs_ref, diff_ref, sems):
    wide, group, rows = dims(hist, local)
    copies = [pltpu.make_async_copy(a, b, sems.at[i]) for i, (a, b) in enumerate(((x_any, x_ref), (f_any, f_ref)))]
    for copy in copies:
        copy.start()
    dirs_ref[...] = jnp.zeros_like(dirs_ref)
    diff_ref[...] = jnp.zeros_like(diff_ref)
    for copy in copies:
        copy.wait()
    delta_f = f_ref[1 : hist + 1, :] - f_ref[0:hist, :]
    delta_x = x_ref[1 : hist + 1, :] - x_ref[0:hist, :]
    last_f = f_ref[hist : hist + 1, :]
    diff_ref[0:hist, :] = delta_f
    diff_ref[hist : hist + 1, :] = last_f
    dirs_ref[0:hist, 0:local] = delta_x + delta_f
    dirs_ref[hist : hist + 1, 0:local] = x_ref[hist : hist + 1, :] + last_f
    gram = lax.dot_general(diff_ref[0:wide, :], diff_ref[...], NT, precision=lax.Precision.HIGHEST, preferred_element_type=F32)
    sub = lax.broadcasted_iota(jnp.int32, gram.shape, 0)
    gram = jnp.where(sub < hist, gram, 0.0)
    flat = jnp.zeros((TILE, LANES), F32)
    for start in range(0, wide, TILE):
        turned = pltpu.roll(gram[start : start + TILE, :], 0, 1, stride=hist + 1, stride_axis=0)
        flat = flat + (pltpu.roll(turned, start * (hist + 1) % LANES, 1) if start else turned)
    message = dirs_ref[pl.ds(0, rows, stride=group), :]
    for place in range(1, group):
        message = message + pltpu.roll(dirs_ref[pl.ds(place, rows, stride=group), :], place * local, 1)
    sub = lax.broadcasted_iota(jnp.int32, message.shape, 0)
    message = jnp.where(sub == rows - 1, jnp.sum(flat, axis=0, keepdims=True), message)
    message = jnp.concatenate([message] * (TILE // rows), axis=0)
    for start in range(0, out_ref.shape[0], TILE):
        out_ref[start : start + TILE, :] = message


def image_kernel(hist, local, row_count, chunk, recv_ref, oper_ref, cat_ref, part_ref, blend_ref, dirs_ref, img_ref):
    wide, group, rows = dims(hist, local)
    row_block, width = oper_ref.shape
    own_rows = row_block // LANES
    mine = recv_ref[pl.ds(pl.multiple_of(lax.axis_index("col") * (row_count * rows), TILE), row_count * rows), :]
    lane = lax.broadcasted_iota(jnp.int32, (rows, LANES), 1)
    for start in range(0, width, LANES):
        for place in range(group):
            spread = jnp.zeros((rows, LANES), F32)
            for slot in range(group):
                block = start // local + slot
                moved = mine[block * rows : (block + 1) * rows, :]
                if slot != place:
                    moved = pltpu.roll(moved, (slot - place) * local % LANES, 1)
                spread = jnp.where(lane // local == slot, moved, spread)
            dirs_ref.at[start // LANES][pl.ds(place, rows, stride=group), :] = spread
    sub = lax.broadcasted_iota(jnp.int32, (wide, width), 0)
    dirs = jnp.concatenate([dirs_ref[i] for i in range(width // LANES)], axis=1)
    dirs = jnp.where(sub <= hist, dirs, 0.0)
    high, low = split(dirs)
    left = jnp.concatenate(
        [jnp.concatenate([high, high], axis=1), jnp.concatenate([low, jnp.zeros_like(low)], axis=1)], axis=0
    )
    for start in range(0, row_block, chunk):
        high, low = split(oper_ref[start : start + chunk, :])
        cat_ref[start : start + chunk, 0:width] = high
        cat_ref[start : start + chunk, width : 2 * width] = low
        both = lax.dot_general(left, jnp.concatenate([high, low], axis=1), NT, preferred_element_type=F32)
        image = both[0:wide, :] + both[wide : 2 * wide, :]
        for piece in range(chunk // LANES):
            tile = image[:, piece * LANES : (piece + 1) * LANES]
            img_ref[pl.ds(start // LANES + piece, hist + 1, stride=own_rows), :] = tile[0 : hist + 1, :]

    flat = jnp.sum(recv_ref[pl.ds(rows - 1, recv_ref.shape[0] // rows, stride=rows), :], axis=0, keepdims=True)
    index = lax.broadcasted_iota(jnp.int32, (wide, LANES), 0)
    gram = jnp.where(index == 0, flat, 0.0)
    for k in range(1, hist):
        gram = jnp.where(index == k, pltpu.roll(flat, LANES - k * (hist + 1), 1), gram)
    cols = [jnp.broadcast_to(gram[:, j : j + 1], (wide, LANES)) for j in range(hist + 1)]

    def row_of(x, k):
        return jnp.broadcast_to(x[k : k + 1, :], (wide, LANES))

    trace = row_of(cols[0], 0)
    for k in range(1, hist):
        trace = trace + row_of(cols[k], k)
    ridge = 0.01 * (trace / hist)
    for k in range(hist):
        cols[k] = jnp.where(index == k, cols[k] + ridge, cols[k])
    for k in range(hist):
        inverse = 1.0 / row_of(cols[k], k)
        for j in range(k + 1, hist + 1):
            ratio = row_of(cols[j], k) * inverse
            cols[j] = jnp.where(index == k, ratio, cols[j] - cols[k] * ratio)
    weights = cols[hist]
    total = img_ref[hist * own_rows : (hist + 1) * own_rows, :]
    for k in range(hist):
        total = total - jnp.broadcast_to(weights[k : k + 1, :], (own_rows, LANES)) * img_ref[k * own_rows : (k + 1) * own_rows, :]
    part_ref[...] = total
    factors = jnp.where(index < hist, -weights, jnp.where(index == hist, 1.0, 0.0))
    for start in range(0, width, LANES):
        blend_ref[:, start : start + LANES] = jnp.sum(factors * dirs[:, start : start + LANES], axis=0, keepdims=True)


def mask_kernel(row_count, ids_ref, target_ref, blend_ref, aux_ref):
    own_rows = aux_ref.shape[1]
    row = lax.axis_index("row")
    first = row * own_rows
    ids = ids_ref[pl.ds(first, own_rows), :]
    before = ids_ref[pl.ds(jnp.maximum(first - 1, 0), 1), :]
    after = ids_ref[pl.ds(jnp.minimum(first + own_rows, ids_ref.shape[0] - 1), 1), :]
    before = jnp.broadcast_to(before[:, LANES - 1 :], (1, LANES))
    after = jnp.broadcast_to(after[:, 0:1], (1, LANES))
    opens = ((ids == before) & (row > 0)).astype(F32)
    aux_ref[TARGET] = target_ref[pl.ds(first, own_rows), :]
    aux_ref[FIRST] = opens
    aux_ref[LAST] = ((ids == after) & (row < row_count - 1)).astype(F32)
    for index, step in enumerate(SHIFTS):
        same = (shifted(ids, step) == ids).astype(F32)
        aux_ref[UPWARD + index] = same
        aux_ref[DOWNWARD + index] = (shifted(ids, -step) == ids).astype(F32)
        if step == 1:
            aux_ref[HEAD] = (1.0 - same) * (1.0 - opens)


def cone_kernel(count, *refs):
    parts = refs[:count]
    aux_ref, cat_ref, proj_ref, edge_ref, out_ref = refs[count:]
    own_rows = proj_ref.shape[0]
    width = out_ref.shape[1]
    slack = aux_ref[TARGET] - tree(p[...] for p in parts)
    head, first, last = aux_ref[HEAD], aux_ref[FIRST], aux_ref[LAST]
    square = (1.0 - head) * slack * slack
    lead, ahead, behind = head * slack, square, square
    for index, step in enumerate(SHIFTS):
        same = aux_ref[UPWARD + index]
        lead = lead + same * shifted(lead, step)
        ahead = ahead + same * shifted(ahead, step)
        behind = behind + aux_ref[DOWNWARD + index] * shifted(behind, -step)
    norm = jnp.sqrt(jnp.maximum(ahead + behind - square, 0.0))
    inside = norm <= lead
    killed = norm <= -lead
    safe = jnp.where(norm > 0, norm, 1.0)
    middle = 0.5 * (lead + norm)
    outside = jnp.where(head > 0, middle, middle * slack / safe)
    projected = jnp.where(inside, slack, jnp.where(killed, 0.0, outside))
    proj_ref[...] = projected
    correction = jnp.where(first + last > 0, 0.0, projected - slack)

    sub = lax.broadcasted_iota(jnp.int32, (TILE, LANES), 0)
    final = own_rows - 1
    begin = (first * slack)[0:1, :]
    tail = (last * (1.0 - head) * slack)[final:, :]
    lead = (last * head)[final:, :]
    closing = jnp.where(sub == TAIL_LAST, tail, jnp.where(sub == HEAD_LAST, lead, 0.0))
    opening = jnp.where(sub == TAIL_FIRST, begin, 0.0)
    pieces = []
    for piece in range(own_rows):
        base = piece // TILE * TILE
        interior = jnp.where(sub == piece % TILE, correction[base : base + TILE, :], 0.0)
        edge = opening if piece == 0 else closing if piece == final else jnp.zeros_like(opening)
        high = jnp.concatenate([interior, edge], axis=0).astype(BF16)
        low = (jnp.concatenate([interior, edge], axis=0) - high.astype(F32)).astype(BF16)
        pieces.append(jnp.concatenate([high, low], axis=0))
    left = jnp.concatenate(pieces, axis=1)
    both = jnp.dot(left, cat_ref[...], preferred_element_type=F32)
    half = 2 * TILE
    sums = both[0:half, 0:width] + both[0:half, width : 2 * width] + both[half : 2 * half, 0:width]
    ends = slack[final:, :]
    scalars = jnp.where(
        sub == SQUARE_LAST,
        tail * ends,
        jnp.where(sub == LEAD_LAST, lead * ends, jnp.where(sub == SQUARE_FIRST, begin * slack[0:1, :], 0.0)),
    )
    scalars = jnp.broadcast_to(jnp.sum(scalars, axis=1, keepdims=True), (TILE, width))
    wide_sub = lax.broadcasted_iota(jnp.int32, (TILE, width), 0)
    out_ref[...] = jnp.where(
        wide_sub == BACK,
        jnp.sum(sums[0:TILE, :], axis=0, keepdims=True),
        jnp.where(wide_sub <= TAIL_FIRST, sums[TILE:half, :], scalars),
    )
    edge_ref[...] = jnp.where(sub == 0, slack[0:1, :], ends)


def finish_kernel(scale_back, local, row_count, *refs):
    messages = refs[:row_count]
    proj_ref, edge_ref, aux_ref, blend_ref, next_ref, out_ref = refs[row_count:]
    row = lax.axis_index("row")
    own_rows, width = proj_ref.shape[0], blend_ref.shape[1]
    received = [m[...] for m in messages]
    blocks = []
    for block in range(row_count):
        mine = received[0]
        for turn in range(1, row_count):
            mine = jnp.where(lax.bitwise_xor(row, turn) == block, received[turn], mine)
        blocks.append(mine)
    total = tree(b[BACK : BACK + 1, :] for b in blocks)
    ones = jnp.ones((1, LANES), F32)
    zeros = jnp.zeros((1, LANES), F32)
    tail_last, lead_last, tail_first = ones, zeros, ones
    for block in range(row_count - 1):
        this, that = blocks[block], blocks[block + 1]
        lead = this[LEAD_LAST : LEAD_LAST + 1, :]
        norm = jnp.sqrt(this[SQUARE_LAST : SQUARE_LAST + 1, :] + that[SQUARE_FIRST : SQUARE_FIRST + 1, :])
        inside = norm <= lead
        killed = norm <= -lead
        safe = jnp.where(norm > 0, norm, 1.0)
        middle = 0.5 * (lead + norm)
        factor = jnp.where(inside, 1.0, jnp.where(killed, 0.0, middle / safe))
        new = jnp.where(inside, lead, jnp.where(killed, 0.0, middle))
        tails = this[TAIL_LAST : TAIL_LAST + 1, :] + that[TAIL_FIRST : TAIL_FIRST + 1, :]
        total = total + ((factor - 1.0) * tails + (new - lead) * this[HEAD_LAST : HEAD_LAST + 1, :])
        tail_last = jnp.where(row == block, factor[:, 0:LANES], tail_last)
        lead_last = jnp.where(row == block, new[:, 0:LANES], lead_last)
        tail_first = jnp.where(row == block + 1, factor[:, 0:LANES], tail_first)
    moved = blend_ref[...] - scale_back * total
    mine = moved[:, 0:local]
    for block in range(1, row_count):
        mine = jnp.where(row == block, moved[:, block * local : (block + 1) * local], mine)
    next_ref[...] = mine
    final = own_rows - 1
    begin, end = edge_ref[0:1, :], edge_ref[1:2, :]
    ahead = jnp.where(aux_ref[FIRST, 0:1, :] > 0, tail_first * begin, proj_ref[0:1, :])
    closing = jnp.where(aux_ref[HEAD, final : final + 1, :] > 0, lead_last, tail_last * end)
    closing = jnp.where(aux_ref[LAST, final : final + 1, :] > 0, closing, proj_ref[final : final + 1, :])
    sub = lax.broadcasted_iota(jnp.int32, (own_rows, LANES), 0)
    out_ref[...] = jnp.where(sub == 0, ahead, jnp.where(sub == final, closing, proj_ref[...]))


def exchange(x, axis, turns):
    count = lax.axis_size(axis)
    return [lax.ppermute(x, axis, [(i, i ^ turn) for i in range(count)]) for turn in turns]


def reduce_col(x, count):
    core = lax.axis_index("col") % 2
    terms, bit = [x, *exchange(x, "col", [1])], 2
    while bit < count:
        x = tree(terms)
        if 2 * bit < count:
            far = lax.ppermute(x, "col", [(i, i ^ (3 * bit if i % 2 else bit)) for i in range(count)])
            near = lax.ppermute(x, "col", [(i, i ^ (2 * bit if i % 2 else bit)) for i in range(count)])
            x = near + jnp.where(core == 1, far, x)
            terms = [x, *exchange(x, "col", [1])]
        else:
            terms = [x, *exchange(x, "col", [bit])]
        bit *= 4
    return terms


def body(iterates, residuals, operator, target, cone_id):
    row_count = lax.axis_size("row")
    col_count = lax.axis_size("col")
    row_block, width = operator.shape
    hist, local = iterates.shape[0] - 1, iterates.shape[1]
    all_rows = row_block * row_count
    scale_back = math.sqrt(local * row_count * col_count / all_rows)
    wide, _, rows = dims(hist, local)
    own_rows = row_block // LANES

    message = pl.pallas_call(
        functools.partial(pack_kernel, hist, local),
        name="pack",
        in_specs=[pl.BlockSpec(memory_space=pltpu.HBM)] * 2,
        out_specs=vmem(),
        out_shape=jax.ShapeDtypeStruct((row_count * col_count * rows, LANES), F32),
        scratch_shapes=[
            pltpu.VMEM((hist + 1, local), F32),
            pltpu.VMEM((hist + 1, local), F32),
            pltpu.VMEM((wide, LANES), F32),
            pltpu.VMEM((LANES, local), F32),
            pltpu.SemaphoreType.DMA((2,)),
        ],
        cost_estimate=pl.CostEstimate(flops=10**10, bytes_accessed=4 * 10**7, transcendentals=0),
        compiler_params=params(),
    )(hbm(iterates), hbm(residuals))
    received = lax.all_to_all(message, ("col", "row"), 0, 0, tiled=True)

    cat, part, blended = pl.pallas_call(
        functools.partial(image_kernel, hist, local, row_count, min(512, row_block)),
        name="image",
        in_specs=[vmem()] * 2,
        out_specs=[vmem()] * 3,
        out_shape=[
            jax.ShapeDtypeStruct((row_block, 2 * width), BF16),
            jax.ShapeDtypeStruct((own_rows, LANES), F32),
            jax.ShapeDtypeStruct((1, width), F32),
        ],
        scratch_shapes=[pltpu.VMEM((width // LANES, wide, LANES), F32), pltpu.VMEM(((hist + 1) * own_rows, LANES), F32)],
        compiler_params=params(),
    )(received, operator)

    aux = pl.pallas_call(
        functools.partial(mask_kernel, row_count),
        name="masks",
        in_specs=[vmem()] * 3,
        out_specs=vmem(),
        out_shape=jax.ShapeDtypeStruct((AUX, own_rows, LANES), F32),
        compiler_params=params(),
    )(cone_id.reshape(-1, LANES), target.reshape(-1, LANES), blended)

    parts = reduce_col(part, col_count)
    projected, edge, back = pl.pallas_call(
        functools.partial(cone_kernel, len(parts)),
        name="cones",
        in_specs=[vmem()] * (len(parts) + 2),
        out_specs=[vmem()] * 3,
        out_shape=[
            jax.ShapeDtypeStruct((own_rows, LANES), F32),
            jax.ShapeDtypeStruct((TILE, LANES), F32),
            jax.ShapeDtypeStruct((TILE, width), F32),
        ],
        compiler_params=params(),
    )(*parts, aux, cat)

    next_point, projected = pl.pallas_call(
        functools.partial(finish_kernel, scale_back, local, row_count),
        name="finish",
        in_specs=[vmem()] * (row_count + 4),
        out_specs=[vmem()] * 2,
        out_shape=[jax.ShapeDtypeStruct((1, local), F32), jax.ShapeDtypeStruct((own_rows, LANES), F32)],
        compiler_params=params(),
    )(back, *exchange(back, "row", range(1, row_count)), projected, edge, aux, blended)
    return (next_point.reshape(local), projected.reshape(row_block))


def solution(mesh):
    return jax.shard_map(
        body,
        mesh=mesh,
        in_specs=(P(None, ("col", "row")), P(None, ("col", "row")), P("row", "col"), P(), P()),
        out_specs=(P(("col", "row")), P("row")),
        check_vma=False,
    )
```

```python
import functools
import math

import jax
import jax.numpy as jnp
from jax import lax
from jax.experimental import pallas as pl
from jax.experimental.pallas import tpu as pltpu
from jax.sharding import PartitionSpec as P

LANES = 128
TILE = 8
BF16 = jnp.bfloat16
F32 = jnp.float32
LIMIT = 24 * 1024 * 1024
SHIFTS = (1, 2, 3, 4, 8, 12)
LEVEL = 3
NT = (((1,), (1,)), ((), ()))
TARGET, HEAD, FIRST, LAST, UPWARD, DOWNWARD = 0, 1, 2, 3, 4, 4 + len(SHIFTS)
AUX = 4 + 2 * len(SHIFTS)
BACK, TAIL_LAST, HEAD_LAST, TAIL_FIRST, SQUARE_LAST, LEAD_LAST, SQUARE_FIRST = range(7)


def params():
    return pltpu.CompilerParams(vmem_limit_bytes=LIMIT)


def vmem():
    return pl.BlockSpec(memory_space=pltpu.VMEM)


def hbm(x):
    return pltpu.with_memory_space_constraint(x, pltpu.HBM)


def tree(terms):
    terms = list(terms)
    while len(terms) > 1:
        terms = [a + b for a, b in zip(terms[::2], terms[1::2])]
    return terms[0]


def split(x):
    high = x.astype(BF16)
    return high, (x - high.astype(F32)).astype(BF16)


def shifted(x, step):
    rows, lanes = x.shape
    lane = lax.broadcasted_iota(jnp.int32, x.shape, 1)
    turned = pltpu.roll(x, step % lanes, 1)
    carried = pltpu.roll(turned, (1 if step > 0 else -1) % rows, 0)
    return jnp.where(lane < step if step > 0 else lane >= lanes + step, carried, turned)


def dims(hist, local):
    wide = -(-(hist + 1) // 16) * 16
    return wide, LANES // local, wide * local // LANES


def pack_kernel(hist, local, x_any, f_any, out_ref, x_ref, f_ref, dirs_ref, diff_ref, sems):
    wide, group, rows = dims(hist, local)
    pieces = -(-hist // TILE)
    copies = [pltpu.make_async_copy(a, b, sems.at[i]) for i, (a, b) in enumerate(((x_any, x_ref), (f_any, f_ref)))]
    for copy in copies:
        copy.start()
    dirs_ref[...] = jnp.zeros_like(dirs_ref)
    diff_ref[...] = jnp.zeros_like(diff_ref)
    for copy in copies:
        copy.wait()
    delta_f = f_ref[1 : hist + 1, :] - f_ref[0:hist, :]
    delta_x = x_ref[1 : hist + 1, :] - x_ref[0:hist, :]
    last_f = f_ref[hist : hist + 1, :]
    for piece in range(pieces):
        base = piece * (LANES + TILE * (hist + 1))
        diff_ref[base : base + hist, :] = delta_f
        diff_ref[base + hist : base + hist + 1, :] = last_f
    dirs_ref[0:hist, 0:local] = delta_x + delta_f
    dirs_ref[hist : hist + 1, 0:local] = x_ref[hist : hist + 1, :] + last_f
    gram = lax.dot_general(diff_ref[0:wide, :], diff_ref[...], NT, precision=lax.Precision.HIGHEST, preferred_element_type=F32)
    sub = lax.broadcasted_iota(jnp.int32, (TILE, LANES), 0)
    flat = jnp.zeros((TILE, LANES), F32)
    for piece in range(pieces):
        block = gram[piece * TILE : (piece + 1) * TILE, piece * LANES : (piece + 1) * LANES]
        block = jnp.where(sub < hist - piece * TILE, block, 0.0)
        flat = flat + pltpu.roll(block, 0, 1, stride=hist + 1, stride_axis=0)
    message = dirs_ref[pl.ds(0, rows, stride=group), :]
    for place in range(1, group):
        message = message + pltpu.roll(dirs_ref[pl.ds(place, rows, stride=group), :], place * local, 1)
    sub = lax.broadcasted_iota(jnp.int32, message.shape, 0)
    message = jnp.where(sub == rows - 1, jnp.sum(flat, axis=0, keepdims=True), message)
    message = jnp.concatenate([message] * (TILE // rows), axis=0)
    for start in range(0, out_ref.shape[0], TILE):
        out_ref[start : start + TILE, :] = message


def image_kernel(hist, local, row_count, chunk, recv_ref, oper_ref, high_ref, low_ref, part_ref, blend_ref, dirs_ref, img_ref):
    wide, group, rows = dims(hist, local)
    row_block, width = oper_ref.shape
    own_rows = row_block // LANES
    mine = recv_ref[pl.ds(pl.multiple_of(lax.axis_index("col") * (row_count * rows), TILE), row_count * rows), :]
    lane = lax.broadcasted_iota(jnp.int32, (rows, LANES), 1)
    for start in range(0, width, LANES):
        for place in range(group):
            spread = jnp.zeros((rows, LANES), F32)
            for slot in range(group):
                block = start // local + slot
                moved = mine[block * rows : (block + 1) * rows, :]
                if slot != place:
                    moved = pltpu.roll(moved, (slot - place) * local % LANES, 1)
                spread = jnp.where(lane // local == slot, moved, spread)
            dirs_ref.at[start // LANES][pl.ds(place, rows, stride=group), :] = spread
    sub = lax.broadcasted_iota(jnp.int32, (wide, width), 0)
    dirs = jnp.concatenate([dirs_ref[i] for i in range(width // LANES)], axis=1)
    dirs = jnp.where(sub <= hist, dirs, 0.0)
    high, low = split(dirs)
    left = jnp.concatenate(
        [jnp.concatenate([high, high], axis=1), jnp.concatenate([low, jnp.zeros_like(low)], axis=1)], axis=0
    )
    for start in range(0, row_block, chunk):
        high, low = split(oper_ref[start : start + chunk, :])
        high_ref[start : start + chunk, :] = high
        low_ref[start : start + chunk, :] = low
        both = lax.dot_general(left, jnp.concatenate([high, low], axis=1), NT, preferred_element_type=F32)
        image = both[0:wide, :] + both[wide : 2 * wide, :]
        for piece in range(chunk // LANES):
            tile = image[:, piece * LANES : (piece + 1) * LANES]
            img_ref[pl.ds(start // LANES + piece, hist + 1, stride=own_rows), :] = tile[0 : hist + 1, :]

    flat = jnp.sum(recv_ref[pl.ds(rows - 1, recv_ref.shape[0] // rows, stride=rows), :], axis=0, keepdims=True)
    index = lax.broadcasted_iota(jnp.int32, (wide, LANES), 0)
    gram = jnp.where(index == 0, flat, 0.0)
    for k in range(1, hist):
        gram = jnp.where(index == k, pltpu.roll(flat, LANES - k * (hist + 1), 1), gram)
    cols = [jnp.broadcast_to(gram[:, j : j + 1], (wide, LANES)) for j in range(hist + 1)]

    def row_of(x, k):
        return jnp.broadcast_to(x[k : k + 1, :], (wide, LANES))

    trace = row_of(cols[0], 0)
    for k in range(1, hist):
        trace = trace + row_of(cols[k], k)
    ridge = 0.01 * (trace / hist)
    for k in range(hist):
        cols[k] = jnp.where(index == k, cols[k] + ridge, cols[k])
    for k in range(hist):
        inverse = 1.0 / row_of(cols[k], k)
        for j in range(k + 1, hist + 1):
            ratio = row_of(cols[j], k) * inverse
            cols[j] = jnp.where(index == k, ratio, cols[j] - cols[k] * ratio)
    weights = cols[hist]
    total = img_ref[hist * own_rows : (hist + 1) * own_rows, :]
    for k in range(hist):
        total = total - jnp.broadcast_to(weights[k : k + 1, :], (own_rows, LANES)) * img_ref[k * own_rows : (k + 1) * own_rows, :]
    part_ref[...] = total
    factors = jnp.where(index < hist, -weights, jnp.where(index == hist, 1.0, 0.0))
    for start in range(0, width, LANES):
        blend_ref[:, start : start + LANES] = jnp.sum(factors * dirs[:, start : start + LANES], axis=0, keepdims=True)


def mask_kernel(row_count, ids_ref, target_ref, blend_ref, aux_ref):
    own_rows = aux_ref.shape[1]
    row = lax.axis_index("row")
    first = row * own_rows
    ids = ids_ref[pl.ds(first, own_rows), :]
    before = ids_ref[pl.ds(jnp.maximum(first - 1, 0), 1), :]
    after = ids_ref[pl.ds(jnp.minimum(first + own_rows, ids_ref.shape[0] - 1), 1), :]
    before = jnp.broadcast_to(before[:, LANES - 1 :], (1, LANES))
    after = jnp.broadcast_to(after[:, 0:1], (1, LANES))
    opens = ((ids == before) & (row > 0)).astype(F32)
    aux_ref[TARGET] = target_ref[pl.ds(first, own_rows), :]
    aux_ref[FIRST] = opens
    aux_ref[LAST] = ((ids == after) & (row < row_count - 1)).astype(F32)
    for index, step in enumerate(SHIFTS):
        same = (shifted(ids, step) == ids).astype(F32)
        aux_ref[UPWARD + index] = same
        aux_ref[DOWNWARD + index] = (shifted(ids, -step) == ids).astype(F32)
        if step == 1:
            aux_ref[HEAD] = (1.0 - same) * (1.0 - opens)


def cone_kernel(count, *refs):
    parts = refs[:count]
    aux_ref, high_ref, low_ref, proj_ref, edge_ref, out_ref = refs[count:]
    own_rows = proj_ref.shape[0]
    width = out_ref.shape[1]
    slack = aux_ref[TARGET] - tree(p[...] for p in parts)
    head, first, last = aux_ref[HEAD], aux_ref[FIRST], aux_ref[LAST]
    square = (1.0 - head) * slack * slack
    lead, ahead, behind = head * slack, square, square
    for level in range(0, len(SHIFTS), LEVEL):
        places = range(level, level + LEVEL)
        lead = lead + sum(aux_ref[UPWARD + i] * shifted(lead, SHIFTS[i]) for i in places)
        ahead = ahead + sum(aux_ref[UPWARD + i] * shifted(ahead, SHIFTS[i]) for i in places)
        behind = behind + sum(aux_ref[DOWNWARD + i] * shifted(behind, -SHIFTS[i]) for i in places)
    norm = jnp.sqrt(jnp.maximum(ahead + behind - square, 0.0))
    inside = norm <= lead
    killed = norm <= -lead
    safe = jnp.where(norm > 0, norm, 1.0)
    middle = 0.5 * (lead + norm)
    outside = jnp.where(head > 0, middle, middle * slack / safe)
    projected = jnp.where(inside, slack, jnp.where(killed, 0.0, outside))
    proj_ref[...] = projected
    correction = jnp.where(first + last > 0, 0.0, projected - slack)

    sub = lax.broadcasted_iota(jnp.int32, (TILE, LANES), 0)
    final = own_rows - 1
    begin = (first * slack)[0:1, :]
    tail = (last * (1.0 - head) * slack)[final:, :]
    lead = (last * head)[final:, :]
    closing = jnp.where(sub == TAIL_LAST, tail, jnp.where(sub == HEAD_LAST, lead, 0.0))
    opening = jnp.where(sub == TAIL_FIRST, begin, 0.0)
    pieces = []
    for piece in range(own_rows):
        base = piece // TILE * TILE
        interior = jnp.where(sub == piece % TILE, correction[base : base + TILE, :], 0.0)
        edge = opening if piece == 0 else closing if piece == final else jnp.zeros_like(opening)
        high = jnp.concatenate([interior, edge], axis=0).astype(BF16)
        low = (jnp.concatenate([interior, edge], axis=0) - high.astype(F32)).astype(BF16)
        pieces.append(jnp.concatenate([high, low], axis=0))
    left = jnp.concatenate(pieces, axis=1)
    both = jnp.dot(left, jnp.concatenate([high_ref[...], low_ref[...]], axis=1), preferred_element_type=F32)
    half = 2 * TILE
    sums = both[0:half, 0:width] + both[0:half, width : 2 * width] + both[half : 2 * half, 0:width]
    ends = slack[final:, :]
    scalars = jnp.where(
        sub == SQUARE_LAST,
        tail * ends,
        jnp.where(sub == LEAD_LAST, lead * ends, jnp.where(sub == SQUARE_FIRST, begin * slack[0:1, :], 0.0)),
    )
    scalars = jnp.broadcast_to(jnp.sum(scalars, axis=1, keepdims=True), (TILE, width))
    wide_sub = lax.broadcasted_iota(jnp.int32, (TILE, width), 0)
    out_ref[...] = jnp.where(
        wide_sub == BACK,
        jnp.sum(sums[0:TILE, :], axis=0, keepdims=True),
        jnp.where(wide_sub <= TAIL_FIRST, sums[TILE:half, :], scalars),
    )
    edge_ref[...] = jnp.where(sub == 0, slack[0:1, :], ends)


def finish_kernel(scale_back, local, row_count, *refs):
    messages = refs[:row_count]
    proj_ref, edge_ref, aux_ref, blend_ref, next_ref, out_ref = refs[row_count:]
    row = lax.axis_index("row")
    own_rows, width = proj_ref.shape[0], blend_ref.shape[1]
    group = LANES // local

    def own_lanes(x):
        mine = x[:, 0:LANES]
        for start in range(1, width // LANES):
            mine = jnp.where(row // group == start, x[:, start * LANES : (start + 1) * LANES], mine)
        return pltpu.roll(mine, (LANES - row % group * local) % LANES, 1)

    def by_block(received):
        blocks = []
        for block in range(row_count):
            mine = received[0]
            for turn in range(1, row_count):
                mine = jnp.where(lax.bitwise_xor(row, turn) == block, received[turn], mine)
            blocks.append(mine)
        return blocks

    received = [m[...] for m in messages]
    scalars = by_block([m[:, 0:LANES] for m in received])
    vectors = by_block([own_lanes(m) for m in received])
    total = tree(b[BACK : BACK + 1, :] for b in vectors)
    ones = jnp.ones((1, LANES), F32)
    zeros = jnp.zeros((1, LANES), F32)
    tail_last, lead_last, tail_first = ones, zeros, ones
    for block in range(row_count - 1):
        this, that = scalars[block], scalars[block + 1]
        lead = this[LEAD_LAST : LEAD_LAST + 1, :]
        norm = jnp.sqrt(this[SQUARE_LAST : SQUARE_LAST + 1, :] + that[SQUARE_FIRST : SQUARE_FIRST + 1, :])
        inside = norm <= lead
        killed = norm <= -lead
        safe = jnp.where(norm > 0, norm, 1.0)
        middle = 0.5 * (lead + norm)
        factor = jnp.where(inside, 1.0, jnp.where(killed, 0.0, middle / safe))
        new = jnp.where(inside, lead, jnp.where(killed, 0.0, middle))
        tails = vectors[block][TAIL_LAST : TAIL_LAST + 1, :] + vectors[block + 1][TAIL_FIRST : TAIL_FIRST + 1, :]
        total = total + ((factor - 1.0) * tails + (new - lead) * vectors[block][HEAD_LAST : HEAD_LAST + 1, :])
        tail_last = jnp.where(row == block, factor, tail_last)
        lead_last = jnp.where(row == block, new, lead_last)
        tail_first = jnp.where(row == block + 1, factor, tail_first)
    next_ref[...] = (own_lanes(blend_ref[...]) - scale_back * total)[:, 0:local]
    final = own_rows - 1
    begin, end = edge_ref[0:1, :], edge_ref[1:2, :]
    ahead = jnp.where(aux_ref[FIRST, 0:1, :] > 0, tail_first * begin, proj_ref[0:1, :])
    closing = jnp.where(aux_ref[HEAD, final : final + 1, :] > 0, lead_last, tail_last * end)
    closing = jnp.where(aux_ref[LAST, final : final + 1, :] > 0, closing, proj_ref[final : final + 1, :])
    sub = lax.broadcasted_iota(jnp.int32, (own_rows, LANES), 0)
    out_ref[...] = jnp.where(sub == 0, ahead, jnp.where(sub == final, closing, proj_ref[...]))


def exchange(x, axis, turns):
    count = lax.axis_size(axis)
    return [lax.ppermute(x, axis, [(i, i ^ turn) for i in range(count)]) for turn in turns]


def reduce_col(x, count):
    core = lax.axis_index("col") % 2
    terms, bit = [x, *exchange(x, "col", [1])], 2
    while bit < count:
        x = tree(terms)
        if 2 * bit < count:
            far = lax.ppermute(x, "col", [(i, i ^ (3 * bit if i % 2 else bit)) for i in range(count)])
            near = lax.ppermute(x, "col", [(i, i ^ (2 * bit if i % 2 else bit)) for i in range(count)])
            x = near + jnp.where(core == 1, far, x)
            terms = [x, *exchange(x, "col", [1])]
        else:
            terms = [x, *exchange(x, "col", [bit])]
        bit *= 4
    return terms


def body(iterates, residuals, operator, target, cone_id):
    row_count = lax.axis_size("row")
    col_count = lax.axis_size("col")
    row_block, width = operator.shape
    hist, local = iterates.shape[0] - 1, iterates.shape[1]
    all_rows = row_block * row_count
    scale_back = math.sqrt(local * row_count * col_count / all_rows)
    wide, _, rows = dims(hist, local)
    own_rows = row_block // LANES

    message = pl.pallas_call(
        functools.partial(pack_kernel, hist, local),
        name="pack",
        in_specs=[pl.BlockSpec(memory_space=pltpu.HBM)] * 2,
        out_specs=vmem(),
        out_shape=jax.ShapeDtypeStruct((row_count * col_count * rows, LANES), F32),
        scratch_shapes=[
            pltpu.VMEM((hist + 1, local), F32),
            pltpu.VMEM((hist + 1, local), F32),
            pltpu.VMEM((wide, LANES), F32),
            pltpu.VMEM((-(-hist // TILE) * LANES, local), F32),
            pltpu.SemaphoreType.DMA((2,)),
        ],
        cost_estimate=pl.CostEstimate(flops=10**10, bytes_accessed=4 * 10**7, transcendentals=0),
        compiler_params=params(),
    )(hbm(iterates), hbm(residuals))
    received = lax.all_to_all(message, ("col", "row"), 0, 0, tiled=True)

    high, low, part, blended = pl.pallas_call(
        functools.partial(image_kernel, hist, local, row_count, min(512, row_block)),
        name="image",
        in_specs=[vmem()] * 2,
        out_specs=[vmem()] * 4,
        out_shape=[
            jax.ShapeDtypeStruct((row_block, width), BF16),
            jax.ShapeDtypeStruct((row_block, width), BF16),
            jax.ShapeDtypeStruct((own_rows, LANES), F32),
            jax.ShapeDtypeStruct((1, width), F32),
        ],
        scratch_shapes=[pltpu.VMEM((width // LANES, wide, LANES), F32), pltpu.VMEM(((hist + 1) * own_rows, LANES), F32)],
        compiler_params=params(),
    )(received, operator)

    aux = pl.pallas_call(
        functools.partial(mask_kernel, row_count),
        name="masks",
        in_specs=[vmem()] * 3,
        out_specs=vmem(),
        out_shape=jax.ShapeDtypeStruct((AUX, own_rows, LANES), F32),
        compiler_params=params(),
    )(cone_id.reshape(-1, LANES), target.reshape(-1, LANES), blended)

    parts = reduce_col(part, col_count)
    projected, edge, back = pl.pallas_call(
        functools.partial(cone_kernel, len(parts)),
        name="cones",
        in_specs=[vmem()] * (len(parts) + 3),
        out_specs=[vmem()] * 3,
        out_shape=[
            jax.ShapeDtypeStruct((own_rows, LANES), F32),
            jax.ShapeDtypeStruct((TILE, LANES), F32),
            jax.ShapeDtypeStruct((TILE, width), F32),
        ],
        compiler_params=params(),
    )(*parts, aux, high, low)

    next_point, projected = pl.pallas_call(
        functools.partial(finish_kernel, scale_back, local, row_count),
        name="finish",
        in_specs=[vmem()] * (row_count + 4),
        out_specs=[vmem()] * 2,
        out_shape=[jax.ShapeDtypeStruct((1, local), F32), jax.ShapeDtypeStruct((own_rows, LANES), F32)],
        compiler_params=params(),
    )(back, *exchange(back, "row", range(1, row_count)), projected, edge, aux, blended)
    return (next_point.reshape(local), projected.reshape(row_block))


def solution(mesh):
    return jax.shard_map(
        body,
        mesh=mesh,
        in_specs=(P(None, ("col", "row")), P(None, ("col", "row")), P("row", "col"), P(), P()),
        out_specs=(P(("col", "row")), P("row")),
        check_vma=False,
    )
```

```python
import functools
import math

import jax
import jax.numpy as jnp
from jax import lax
from jax.experimental import pallas as pl
from jax.experimental.pallas import tpu as pltpu
from jax.sharding import PartitionSpec as P

LANES = 128
TILE = 8
BF16 = jnp.bfloat16
F32 = jnp.float32
LIMIT = 32 * 1024 * 1024
SHIFTS = (1, 2, 3, 4, 8, 12)
LEVEL = 3
NT = (((1,), (1,)), ((), ()))
TARGET, HEAD, FIRST, LAST, UPWARD, DOWNWARD = 0, 1, 2, 3, 4, 4 + len(SHIFTS)
AUX = 4 + 2 * len(SHIFTS)
BACK, TAIL_LAST, HEAD_LAST, TAIL_FIRST, SQUARE_LAST, LEAD_LAST, SQUARE_FIRST = range(7)


def params():
    return pltpu.CompilerParams(vmem_limit_bytes=LIMIT)


def vmem():
    return pl.BlockSpec(memory_space=pltpu.VMEM)


def hbm(x):
    return pltpu.with_memory_space_constraint(x, pltpu.HBM)


def tree(terms):
    terms = list(terms)
    while len(terms) > 1:
        terms = [a + b for a, b in zip(terms[::2], terms[1::2])]
    return terms[0]


def split(x):
    high = x.astype(BF16)
    return high, (x - high.astype(F32)).astype(BF16)


def shifted(x, step):
    rows, lanes = x.shape
    lane = lax.broadcasted_iota(jnp.int32, x.shape, 1)
    turned = pltpu.roll(x, step % lanes, 1)
    carried = pltpu.roll(turned, (1 if step > 0 else -1) % rows, 0)
    return jnp.where(lane < step if step > 0 else lane >= lanes + step, carried, turned)


def dims(hist, local):
    wide = -(-(hist + 1) // 16) * 16
    return wide, LANES // local, wide * local // LANES


def pack_kernel(hist, local, x_any, f_any, out_ref, x_ref, f_ref, dirs_ref, diff_ref, sems):
    wide, group, rows = dims(hist, local)
    pieces = -(-hist // TILE)
    copies = [pltpu.make_async_copy(a, b, sems.at[i]) for i, (a, b) in enumerate(((x_any, x_ref), (f_any, f_ref)))]
    for copy in copies:
        copy.start()
    dirs_ref[...] = jnp.zeros_like(dirs_ref)
    diff_ref[...] = jnp.zeros_like(diff_ref)
    for copy in copies:
        copy.wait()
    delta_f = f_ref[1 : hist + 1, :] - f_ref[0:hist, :]
    delta_x = x_ref[1 : hist + 1, :] - x_ref[0:hist, :]
    last_f = f_ref[hist : hist + 1, :]
    for piece in range(pieces):
        base = piece * (LANES + TILE * (hist + 1))
        diff_ref[base : base + hist, :] = delta_f
        diff_ref[base + hist : base + hist + 1, :] = last_f
    dirs_ref[0:hist, 0:local] = delta_x + delta_f
    dirs_ref[hist : hist + 1, 0:local] = x_ref[hist : hist + 1, :] + last_f
    gram = lax.dot_general(diff_ref[0:wide, :], diff_ref[...], NT, precision=lax.Precision.HIGHEST, preferred_element_type=F32)
    sub = lax.broadcasted_iota(jnp.int32, (TILE, LANES), 0)
    flat = jnp.zeros((TILE, LANES), F32)
    for piece in range(pieces):
        block = gram[piece * TILE : (piece + 1) * TILE, piece * LANES : (piece + 1) * LANES]
        block = jnp.where(sub < hist - piece * TILE, block, 0.0)
        flat = flat + pltpu.roll(block, 0, 1, stride=hist + 1, stride_axis=0)
    message = dirs_ref[pl.ds(0, rows, stride=group), :]
    for place in range(1, group):
        message = message + pltpu.roll(dirs_ref[pl.ds(place, rows, stride=group), :], place * local, 1)
    sub = lax.broadcasted_iota(jnp.int32, message.shape, 0)
    message = jnp.where(sub == rows - 1, jnp.sum(flat, axis=0, keepdims=True), message)
    message = jnp.concatenate([message] * (TILE // rows), axis=0)
    for start in range(0, out_ref.shape[0], TILE):
        out_ref[start : start + TILE, :] = message


def directions(hist, local, row_count, col, recv_ref, dirs_ref):
    wide, group, rows = dims(hist, local)
    mine = recv_ref[pl.ds(pl.multiple_of(col * (row_count * rows), TILE), row_count * rows), :]
    lane = lax.broadcasted_iota(jnp.int32, (rows, LANES), 1)
    width = row_count * local
    for start in range(0, width, LANES):
        for place in range(group):
            spread = jnp.zeros((rows, LANES), F32)
            for slot in range(group):
                block = start // local + slot
                moved = mine[block * rows : (block + 1) * rows, :]
                if slot != place:
                    moved = pltpu.roll(moved, (slot - place) * local % LANES, 1)
                spread = jnp.where(lane // local == slot, moved, spread)
            dirs_ref.at[start // LANES][pl.ds(place, rows, stride=group), :] = spread
    sub = lax.broadcasted_iota(jnp.int32, (wide, width), 0)
    dirs = jnp.concatenate([dirs_ref[i] for i in range(width // LANES)], axis=1)
    return jnp.where(sub <= hist, dirs, 0.0)


def left_operand(dirs):
    high, low = split(dirs)
    return jnp.concatenate(
        [jnp.concatenate([high, high], axis=1), jnp.concatenate([low, jnp.zeros_like(low)], axis=1)], axis=0
    )


def image_kernel(hist, local, row_count, chunk, recv_ref, *refs):
    oper_ref, other_ref, high_ref, low_ref, part_ref, blend_ref, dirs_ref, far_ref, img_ref = refs
    wide, _, rows = dims(hist, local)
    row_block, width = oper_ref.shape
    own_rows = row_block // LANES
    col = lax.axis_index("col")
    dirs = directions(hist, local, row_count, col, recv_ref, dirs_ref)
    left = left_operand(dirs)
    far = left_operand(directions(hist, local, row_count, lax.bitwise_xor(col, 1), recv_ref, far_ref))

    def multiply(left, high, low):
        both = lax.dot_general(left, jnp.concatenate([high, low], axis=1), NT, preferred_element_type=F32)
        return both[0:wide, :] + both[wide : 2 * wide, :]

    for start in range(0, row_block, chunk):
        high, low = split(oper_ref[start : start + chunk, :])
        high_ref[start : start + chunk, :] = high
        low_ref[start : start + chunk, :] = low
        image = multiply(left, high, low) + multiply(far, *split(other_ref[start : start + chunk, :]))
        for piece in range(chunk // LANES):
            tile = image[:, piece * LANES : (piece + 1) * LANES]
            img_ref[pl.ds(start // LANES + piece, hist + 1, stride=own_rows), :] = tile[0 : hist + 1, :]

    flat = jnp.sum(recv_ref[pl.ds(rows - 1, recv_ref.shape[0] // rows, stride=rows), :], axis=0, keepdims=True)
    index = lax.broadcasted_iota(jnp.int32, (wide, LANES), 0)
    gram = jnp.where(index == 0, flat, 0.0)
    for k in range(1, hist):
        gram = jnp.where(index == k, pltpu.roll(flat, LANES - k * (hist + 1), 1), gram)
    cols = [jnp.broadcast_to(gram[:, j : j + 1], (wide, LANES)) for j in range(hist + 1)]

    def row_of(x, k):
        return jnp.broadcast_to(x[k : k + 1, :], (wide, LANES))

    trace = row_of(cols[0], 0)
    for k in range(1, hist):
        trace = trace + row_of(cols[k], k)
    ridge = 0.01 * (trace / hist)
    for k in range(hist):
        cols[k] = jnp.where(index == k, cols[k] + ridge, cols[k])
    for k in range(hist):
        inverse = 1.0 / row_of(cols[k], k)
        for j in range(k + 1, hist + 1):
            ratio = row_of(cols[j], k) * inverse
            cols[j] = jnp.where(index == k, ratio, cols[j] - cols[k] * ratio)
    weights = cols[hist]
    total = img_ref[hist * own_rows : (hist + 1) * own_rows, :]
    for k in range(hist):
        total = total - jnp.broadcast_to(weights[k : k + 1, :], (own_rows, LANES)) * img_ref[k * own_rows : (k + 1) * own_rows, :]
    part_ref[...] = total
    factors = jnp.where(index < hist, -weights, jnp.where(index == hist, 1.0, 0.0))
    for start in range(0, width, LANES):
        blend_ref[:, start : start + LANES] = jnp.sum(factors * dirs[:, start : start + LANES], axis=0, keepdims=True)


def mask_kernel(row_count, ids_ref, target_ref, blend_ref, aux_ref):
    own_rows = aux_ref.shape[1]
    row = lax.axis_index("row")
    first = row * own_rows
    ids = ids_ref[pl.ds(first, own_rows), :]
    before = ids_ref[pl.ds(jnp.maximum(first - 1, 0), 1), :]
    after = ids_ref[pl.ds(jnp.minimum(first + own_rows, ids_ref.shape[0] - 1), 1), :]
    before = jnp.broadcast_to(before[:, LANES - 1 :], (1, LANES))
    after = jnp.broadcast_to(after[:, 0:1], (1, LANES))
    opens = ((ids == before) & (row > 0)).astype(F32)
    aux_ref[TARGET] = target_ref[pl.ds(first, own_rows), :]
    aux_ref[FIRST] = opens
    aux_ref[LAST] = ((ids == after) & (row < row_count - 1)).astype(F32)
    for index, step in enumerate(SHIFTS):
        same = (shifted(ids, step) == ids).astype(F32)
        aux_ref[UPWARD + index] = same
        aux_ref[DOWNWARD + index] = (shifted(ids, -step) == ids).astype(F32)
        if step == 1:
            aux_ref[HEAD] = (1.0 - same) * (1.0 - opens)


def cone_kernel(count, *refs):
    parts = refs[:count]
    aux_ref, high_ref, low_ref, proj_ref, edge_ref, out_ref = refs[count:]
    own_rows = proj_ref.shape[0]
    width = out_ref.shape[1]
    slack = aux_ref[TARGET] - tree(p[...] for p in parts)
    head, first, last = aux_ref[HEAD], aux_ref[FIRST], aux_ref[LAST]
    square = (1.0 - head) * slack * slack
    lead, ahead, behind = head * slack, square, square
    for level in range(0, len(SHIFTS), LEVEL):
        places = range(level, level + LEVEL)
        lead = lead + sum(aux_ref[UPWARD + i] * shifted(lead, SHIFTS[i]) for i in places)
        ahead = ahead + sum(aux_ref[UPWARD + i] * shifted(ahead, SHIFTS[i]) for i in places)
        behind = behind + sum(aux_ref[DOWNWARD + i] * shifted(behind, -SHIFTS[i]) for i in places)
    norm = jnp.sqrt(jnp.maximum(ahead + behind - square, 0.0))
    inside = norm <= lead
    killed = norm <= -lead
    safe = jnp.where(norm > 0, norm, 1.0)
    middle = 0.5 * (lead + norm)
    outside = jnp.where(head > 0, middle, middle * slack / safe)
    projected = jnp.where(inside, slack, jnp.where(killed, 0.0, outside))
    proj_ref[...] = projected
    correction = jnp.where(first + last > 0, 0.0, projected - slack)

    sub = lax.broadcasted_iota(jnp.int32, (TILE, LANES), 0)
    final = own_rows - 1
    begin = (first * slack)[0:1, :]
    tail = (last * (1.0 - head) * slack)[final:, :]
    lead = (last * head)[final:, :]
    closing = jnp.where(sub == TAIL_LAST, tail, jnp.where(sub == HEAD_LAST, lead, 0.0))
    opening = jnp.where(sub == TAIL_FIRST, begin, 0.0)
    pieces = []
    for piece in range(own_rows):
        base = piece // TILE * TILE
        interior = jnp.where(sub == piece % TILE, correction[base : base + TILE, :], 0.0)
        edge = opening if piece == 0 else closing if piece == final else jnp.zeros_like(opening)
        high = jnp.concatenate([interior, edge], axis=0).astype(BF16)
        low = (jnp.concatenate([interior, edge], axis=0) - high.astype(F32)).astype(BF16)
        pieces.append(jnp.concatenate([high, low], axis=0))
    left = jnp.concatenate(pieces, axis=1)
    both = jnp.dot(left, jnp.concatenate([high_ref[...], low_ref[...]], axis=1), preferred_element_type=F32)
    half = 2 * TILE
    sums = both[0:half, 0:width] + both[0:half, width : 2 * width] + both[half : 2 * half, 0:width]
    ends = slack[final:, :]
    scalars = jnp.where(
        sub == SQUARE_LAST,
        tail * ends,
        jnp.where(sub == LEAD_LAST, lead * ends, jnp.where(sub == SQUARE_FIRST, begin * slack[0:1, :], 0.0)),
    )
    scalars = jnp.broadcast_to(jnp.sum(scalars, axis=1, keepdims=True), (TILE, width))
    wide_sub = lax.broadcasted_iota(jnp.int32, (TILE, width), 0)
    out_ref[...] = jnp.where(
        wide_sub == BACK,
        jnp.sum(sums[0:TILE, :], axis=0, keepdims=True),
        jnp.where(wide_sub <= TAIL_FIRST, sums[TILE:half, :], scalars),
    )
    edge_ref[...] = jnp.where(sub == 0, slack[0:1, :], ends)


def finish_kernel(scale_back, local, row_count, *refs):
    messages = refs[:row_count]
    proj_ref, edge_ref, aux_ref, blend_ref, next_ref, out_ref = refs[row_count:]
    row = lax.axis_index("row")
    own_rows, width = proj_ref.shape[0], blend_ref.shape[1]
    group = LANES // local

    def own_lanes(x):
        mine = x[:, 0:LANES]
        for start in range(1, width // LANES):
            mine = jnp.where(row // group == start, x[:, start * LANES : (start + 1) * LANES], mine)
        return pltpu.roll(mine, (LANES - row % group * local) % LANES, 1)

    def by_block(received):
        blocks = []
        for block in range(row_count):
            mine = received[0]
            for turn in range(1, row_count):
                mine = jnp.where(lax.bitwise_xor(row, turn) == block, received[turn], mine)
            blocks.append(mine)
        return blocks

    received = [m[...] for m in messages]
    scalars = by_block([m[:, 0:LANES] for m in received])
    vectors = by_block([own_lanes(m) for m in received])
    total = tree(b[BACK : BACK + 1, :] for b in vectors)
    ones = jnp.ones((1, LANES), F32)
    zeros = jnp.zeros((1, LANES), F32)
    tail_last, lead_last, tail_first = ones, zeros, ones
    for block in range(row_count - 1):
        this, that = scalars[block], scalars[block + 1]
        lead = this[LEAD_LAST : LEAD_LAST + 1, :]
        norm = jnp.sqrt(this[SQUARE_LAST : SQUARE_LAST + 1, :] + that[SQUARE_FIRST : SQUARE_FIRST + 1, :])
        inside = norm <= lead
        killed = norm <= -lead
        safe = jnp.where(norm > 0, norm, 1.0)
        middle = 0.5 * (lead + norm)
        factor = jnp.where(inside, 1.0, jnp.where(killed, 0.0, middle / safe))
        new = jnp.where(inside, lead, jnp.where(killed, 0.0, middle))
        tails = vectors[block][TAIL_LAST : TAIL_LAST + 1, :] + vectors[block + 1][TAIL_FIRST : TAIL_FIRST + 1, :]
        total = total + ((factor - 1.0) * tails + (new - lead) * vectors[block][HEAD_LAST : HEAD_LAST + 1, :])
        tail_last = jnp.where(row == block, factor, tail_last)
        lead_last = jnp.where(row == block, new, lead_last)
        tail_first = jnp.where(row == block + 1, factor, tail_first)
    next_ref[...] = (own_lanes(blend_ref[...]) - scale_back * total)[:, 0:local]
    final = own_rows - 1
    begin, end = edge_ref[0:1, :], edge_ref[1:2, :]
    ahead = jnp.where(aux_ref[FIRST, 0:1, :] > 0, tail_first * begin, proj_ref[0:1, :])
    closing = jnp.where(aux_ref[HEAD, final : final + 1, :] > 0, lead_last, tail_last * end)
    closing = jnp.where(aux_ref[LAST, final : final + 1, :] > 0, closing, proj_ref[final : final + 1, :])
    sub = lax.broadcasted_iota(jnp.int32, (own_rows, LANES), 0)
    out_ref[...] = jnp.where(sub == 0, ahead, jnp.where(sub == final, closing, proj_ref[...]))


def exchange(x, axis, turns):
    count = lax.axis_size(axis)
    return [lax.ppermute(x, axis, [(i, i ^ turn) for i in range(count)]) for turn in turns]


def reduce_chips(x, count):
    core = lax.axis_index("col") % 2
    terms, bit = [x], 2
    while bit < count:
        x = tree(terms)
        if 2 * bit < count:
            far = lax.ppermute(x, "col", [(i, i ^ (3 * bit if i % 2 else bit)) for i in range(count)])
            near = lax.ppermute(x, "col", [(i, i ^ (2 * bit if i % 2 else bit)) for i in range(count)])
            x = near + jnp.where(core == 1, far, x)
            terms = [x, *exchange(x, "col", [1])]
        else:
            terms = [x, *exchange(x, "col", [bit])]
        bit *= 4
    return terms


def body(iterates, residuals, operator, target, cone_id):
    row_count = lax.axis_size("row")
    col_count = lax.axis_size("col")
    row_block, width = operator.shape
    hist, local = iterates.shape[0] - 1, iterates.shape[1]
    all_rows = row_block * row_count
    scale_back = math.sqrt(local * row_count * col_count / all_rows)
    wide, _, rows = dims(hist, local)
    own_rows = row_block // LANES

    (other,) = exchange(operator, "col", [1])
    message = pl.pallas_call(
        functools.partial(pack_kernel, hist, local),
        name="pack",
        in_specs=[pl.BlockSpec(memory_space=pltpu.HBM)] * 2,
        out_specs=vmem(),
        out_shape=jax.ShapeDtypeStruct((row_count * col_count * rows, LANES), F32),
        scratch_shapes=[
            pltpu.VMEM((hist + 1, local), F32),
            pltpu.VMEM((hist + 1, local), F32),
            pltpu.VMEM((wide, LANES), F32),
            pltpu.VMEM((-(-hist // TILE) * LANES, local), F32),
            pltpu.SemaphoreType.DMA((2,)),
        ],
        cost_estimate=pl.CostEstimate(flops=10**10, bytes_accessed=4 * 10**7, transcendentals=0),
        compiler_params=params(),
    )(hbm(iterates), hbm(residuals))
    received = lax.all_to_all(message, ("col", "row"), 0, 0, tiled=True)

    high, low, part, blended = pl.pallas_call(
        functools.partial(image_kernel, hist, local, row_count, min(512, row_block)),
        name="image",
        in_specs=[vmem()] * 3,
        out_specs=[vmem()] * 4,
        out_shape=[
            jax.ShapeDtypeStruct((row_block, width), BF16),
            jax.ShapeDtypeStruct((row_block, width), BF16),
            jax.ShapeDtypeStruct((own_rows, LANES), F32),
            jax.ShapeDtypeStruct((1, width), F32),
        ],
        scratch_shapes=[
            pltpu.VMEM((width // LANES, wide, LANES), F32),
            pltpu.VMEM((width // LANES, wide, LANES), F32),
            pltpu.VMEM(((hist + 1) * own_rows, LANES), F32),
        ],
        compiler_params=params(),
    )(received, operator, other)

    aux = pl.pallas_call(
        functools.partial(mask_kernel, row_count),
        name="masks",
        in_specs=[vmem()] * 3,
        out_specs=vmem(),
        out_shape=jax.ShapeDtypeStruct((AUX, own_rows, LANES), F32),
        compiler_params=params(),
    )(cone_id.reshape(-1, LANES), target.reshape(-1, LANES), blended)

    parts = reduce_chips(part, col_count)
    projected, edge, back = pl.pallas_call(
        functools.partial(cone_kernel, len(parts)),
        name="cones",
        in_specs=[vmem()] * (len(parts) + 3),
        out_specs=[vmem()] * 3,
        out_shape=[
            jax.ShapeDtypeStruct((own_rows, LANES), F32),
            jax.ShapeDtypeStruct((TILE, LANES), F32),
            jax.ShapeDtypeStruct((TILE, width), F32),
        ],
        compiler_params=params(),
    )(*parts, aux, high, low)

    next_point, projected = pl.pallas_call(
        functools.partial(finish_kernel, scale_back, local, row_count),
        name="finish",
        in_specs=[vmem()] * (row_count + 4),
        out_specs=[vmem()] * 2,
        out_shape=[jax.ShapeDtypeStruct((1, local), F32), jax.ShapeDtypeStruct((own_rows, LANES), F32)],
        compiler_params=params(),
    )(back, *exchange(back, "row", range(1, row_count)), projected, edge, aux, blended)
    return (next_point.reshape(local), projected.reshape(row_block))


def solution(mesh):
    return jax.shard_map(
        body,
        mesh=mesh,
        in_specs=(P(None, ("col", "row")), P(None, ("col", "row")), P("row", "col"), P(), P()),
        out_specs=(P(("col", "row")), P("row")),
        check_vma=False,
    )
```

```python
import functools
import math

import jax
import jax.numpy as jnp
from jax import lax
from jax.experimental import pallas as pl
from jax.experimental.pallas import tpu as pltpu
from jax.sharding import PartitionSpec as P

LANES = 128
TILE = 8
BF16 = jnp.bfloat16
F32 = jnp.float32
SMALL = 8 * 1024 * 1024
SHIFTS = (1, 2, 3, 4, 8, 12)
LEVEL = 3
NT = (((1,), (1,)), ((), ()))
TARGET, HEAD, FIRST, LAST, UPWARD, DOWNWARD = 0, 1, 2, 3, 4, 4 + len(SHIFTS)
AUX = 4 + 2 * len(SHIFTS)
BACK, TAIL_LAST, HEAD_LAST, TAIL_FIRST, SQUARE_LAST, LEAD_LAST, SQUARE_FIRST = range(7)


def params(blocks=0):
    return pltpu.CompilerParams(vmem_limit_bytes=SMALL + blocks)


def vmem():
    return pl.BlockSpec(memory_space=pltpu.VMEM)


def hbm(x):
    return pltpu.with_memory_space_constraint(x, pltpu.HBM)


def tree(terms):
    terms = list(terms)
    while len(terms) > 1:
        terms = [a + b for a, b in zip(terms[::2], terms[1::2])]
    return terms[0]


def split(x):
    high = x.astype(BF16)
    return high, (x - high.astype(F32)).astype(BF16)


def shifted(x, step):
    rows, lanes = x.shape
    lane = lax.broadcasted_iota(jnp.int32, x.shape, 1)
    turned = pltpu.roll(x, step % lanes, 1)
    carried = pltpu.roll(turned, (1 if step > 0 else -1) % rows, 0)
    return jnp.where(lane < step if step > 0 else lane >= lanes + step, carried, turned)


def dims(hist, local):
    wide = -(-(hist + 1) // 16) * 16
    return wide, LANES // local, wide * local // LANES


def pack_kernel(hist, local, x_any, f_any, out_ref, x_ref, f_ref, dirs_ref, diff_ref, sems):
    wide, group, rows = dims(hist, local)
    pieces = -(-hist // TILE)
    copies = [pltpu.make_async_copy(a, b, sems.at[i]) for i, (a, b) in enumerate(((x_any, x_ref), (f_any, f_ref)))]
    for copy in copies:
        copy.start()
    dirs_ref[...] = jnp.zeros_like(dirs_ref)
    diff_ref[...] = jnp.zeros_like(diff_ref)
    for copy in copies:
        copy.wait()
    delta_f = f_ref[1 : hist + 1, :] - f_ref[0:hist, :]
    delta_x = x_ref[1 : hist + 1, :] - x_ref[0:hist, :]
    last_f = f_ref[hist : hist + 1, :]
    for piece in range(pieces):
        base = piece * (LANES + TILE * (hist + 1))
        diff_ref[base : base + hist, :] = delta_f
        diff_ref[base + hist : base + hist + 1, :] = last_f
    dirs_ref[0:hist, 0:local] = delta_x + delta_f
    dirs_ref[hist : hist + 1, 0:local] = x_ref[hist : hist + 1, :] + last_f
    gram = lax.dot_general(diff_ref[0:wide, :], diff_ref[...], NT, precision=lax.Precision.HIGHEST, preferred_element_type=F32)
    sub = lax.broadcasted_iota(jnp.int32, (TILE, LANES), 0)
    flat = jnp.zeros((TILE, LANES), F32)
    for piece in range(pieces):
        block = gram[piece * TILE : (piece + 1) * TILE, piece * LANES : (piece + 1) * LANES]
        block = jnp.where(sub < hist - piece * TILE, block, 0.0)
        flat = flat + pltpu.roll(block, 0, 1, stride=hist + 1, stride_axis=0)
    message = dirs_ref[pl.ds(0, rows, stride=group), :]
    for place in range(1, group):
        message = message + pltpu.roll(dirs_ref[pl.ds(place, rows, stride=group), :], place * local, 1)
    sub = lax.broadcasted_iota(jnp.int32, message.shape, 0)
    message = jnp.where(sub == rows - 1, jnp.sum(flat, axis=0, keepdims=True), message)
    message = jnp.concatenate([message] * (TILE // rows), axis=0)
    for start in range(0, out_ref.shape[0], TILE):
        out_ref[start : start + TILE, :] = message


def directions(hist, local, row_count, col, recv_ref, dirs_ref):
    wide, group, rows = dims(hist, local)
    mine = recv_ref[pl.ds(pl.multiple_of(col * (row_count * rows), TILE), row_count * rows), :]
    lane = lax.broadcasted_iota(jnp.int32, (rows, LANES), 1)
    width = row_count * local
    for start in range(0, width, LANES):
        for place in range(group):
            spread = jnp.zeros((rows, LANES), F32)
            for slot in range(group):
                block = start // local + slot
                moved = mine[block * rows : (block + 1) * rows, :]
                if slot != place:
                    moved = pltpu.roll(moved, (slot - place) * local % LANES, 1)
                spread = jnp.where(lane // local == slot, moved, spread)
            dirs_ref.at[start // LANES][pl.ds(place, rows, stride=group), :] = spread
    sub = lax.broadcasted_iota(jnp.int32, (wide, width), 0)
    dirs = jnp.concatenate([dirs_ref[i] for i in range(width // LANES)], axis=1)
    return jnp.where(sub <= hist, dirs, 0.0)


def left_operand(dirs):
    high, low = split(dirs)
    return jnp.concatenate(
        [jnp.concatenate([high, high], axis=1), jnp.concatenate([low, jnp.zeros_like(low)], axis=1)], axis=0
    )


def image_kernel(hist, local, row_count, chunk, recv_ref, *refs):
    oper_ref, other_ref, *split_refs, part_ref, blend_ref, dirs_ref, far_ref, img_ref = refs
    wide, _, rows = dims(hist, local)
    row_block, width = oper_ref.shape
    own_rows = row_block // LANES
    col = lax.axis_index("col")
    dirs = directions(hist, local, row_count, col, recv_ref, dirs_ref)
    left = left_operand(dirs)
    far = left_operand(directions(hist, local, row_count, lax.bitwise_xor(col, 1), recv_ref, far_ref))

    def multiply(left, high, low):
        both = lax.dot_general(left, jnp.concatenate([high, low], axis=1), NT, preferred_element_type=F32)
        return both[0:wide, :] + both[wide : 2 * wide, :]

    for start in range(0, row_block, chunk):
        own = split(oper_ref[start : start + chunk, :])
        other = split(other_ref[start : start + chunk, :])
        for ref, value in zip(split_refs, (*own, *other)):
            ref[start : start + chunk, :] = value
        image = multiply(left, *own) + multiply(far, *other)
        for piece in range(chunk // LANES):
            tile = image[:, piece * LANES : (piece + 1) * LANES]
            img_ref[pl.ds(start // LANES + piece, hist + 1, stride=own_rows), :] = tile[0 : hist + 1, :]

    flat = jnp.sum(recv_ref[pl.ds(rows - 1, recv_ref.shape[0] // rows, stride=rows), :], axis=0, keepdims=True)
    index = lax.broadcasted_iota(jnp.int32, (wide, LANES), 0)
    gram = jnp.where(index == 0, flat, 0.0)
    for k in range(1, hist):
        gram = jnp.where(index == k, pltpu.roll(flat, LANES - k * (hist + 1), 1), gram)
    cols = [jnp.broadcast_to(gram[:, j : j + 1], (wide, LANES)) for j in range(hist + 1)]

    def row_of(x, k):
        return jnp.broadcast_to(x[k : k + 1, :], (wide, LANES))

    trace = row_of(cols[0], 0)
    for k in range(1, hist):
        trace = trace + row_of(cols[k], k)
    ridge = 0.01 * (trace / hist)
    for k in range(hist):
        cols[k] = jnp.where(index == k, cols[k] + ridge, cols[k])
    for k in range(hist):
        inverse = 1.0 / row_of(cols[k], k)
        for j in range(k + 1, hist + 1):
            ratio = row_of(cols[j], k) * inverse
            cols[j] = jnp.where(index == k, ratio, cols[j] - cols[k] * ratio)
    weights = cols[hist]
    total = img_ref[hist * own_rows : (hist + 1) * own_rows, :]
    for k in range(hist):
        total = total - jnp.broadcast_to(weights[k : k + 1, :], (own_rows, LANES)) * img_ref[k * own_rows : (k + 1) * own_rows, :]
    part_ref[...] = total
    factors = jnp.where(index < hist, -weights, jnp.where(index == hist, 1.0, 0.0))
    for start in range(0, width, LANES):
        blend_ref[:, start : start + LANES] = jnp.sum(factors * dirs[:, start : start + LANES], axis=0, keepdims=True)


def mask_kernel(row_count, ids_ref, target_ref, blend_ref, aux_ref):
    own_rows = aux_ref.shape[1]
    row = lax.axis_index("row")
    first = row * own_rows
    ids = ids_ref[pl.ds(first, own_rows), :]
    before = ids_ref[pl.ds(jnp.maximum(first - 1, 0), 1), :]
    after = ids_ref[pl.ds(jnp.minimum(first + own_rows, ids_ref.shape[0] - 1), 1), :]
    before = jnp.broadcast_to(before[:, LANES - 1 :], (1, LANES))
    after = jnp.broadcast_to(after[:, 0:1], (1, LANES))
    opens = ((ids == before) & (row > 0)).astype(F32)
    aux_ref[TARGET] = target_ref[pl.ds(first, own_rows), :]
    aux_ref[FIRST] = opens
    aux_ref[LAST] = ((ids == after) & (row < row_count - 1)).astype(F32)
    for index, step in enumerate(SHIFTS):
        same = (shifted(ids, step) == ids).astype(F32)
        aux_ref[UPWARD + index] = same
        aux_ref[DOWNWARD + index] = (shifted(ids, -step) == ids).astype(F32)
        if step == 1:
            aux_ref[HEAD] = (1.0 - same) * (1.0 - opens)


def cone_kernel(count, *refs):
    parts = refs[:count]
    aux_ref, *split_refs, proj_ref, edge_ref, own_ref, other_ref = refs[count:]
    own_rows = proj_ref.shape[0]
    width = own_ref.shape[1]
    slack = aux_ref[TARGET] - tree(p[...] for p in parts)
    head, first, last = aux_ref[HEAD], aux_ref[FIRST], aux_ref[LAST]
    square = (1.0 - head) * slack * slack
    lead, ahead, behind = head * slack, square, square
    for level in range(0, len(SHIFTS), LEVEL):
        places = range(level, level + LEVEL)
        lead = lead + sum(aux_ref[UPWARD + i] * shifted(lead, SHIFTS[i]) for i in places)
        ahead = ahead + sum(aux_ref[UPWARD + i] * shifted(ahead, SHIFTS[i]) for i in places)
        behind = behind + sum(aux_ref[DOWNWARD + i] * shifted(behind, -SHIFTS[i]) for i in places)
    norm = jnp.sqrt(jnp.maximum(ahead + behind - square, 0.0))
    inside = norm <= lead
    killed = norm <= -lead
    safe = jnp.where(norm > 0, norm, 1.0)
    middle = 0.5 * (lead + norm)
    outside = jnp.where(head > 0, middle, middle * slack / safe)
    projected = jnp.where(inside, slack, jnp.where(killed, 0.0, outside))
    proj_ref[...] = projected
    correction = jnp.where(first + last > 0, 0.0, projected - slack)

    sub = lax.broadcasted_iota(jnp.int32, (TILE, LANES), 0)
    final = own_rows - 1
    begin = (first * slack)[0:1, :]
    tail = (last * (1.0 - head) * slack)[final:, :]
    lead = (last * head)[final:, :]
    closing = jnp.where(sub == TAIL_LAST, tail, jnp.where(sub == HEAD_LAST, lead, 0.0))
    opening = jnp.where(sub == TAIL_FIRST, begin, 0.0)
    pieces = []
    for piece in range(own_rows):
        base = piece // TILE * TILE
        interior = jnp.where(sub == piece % TILE, correction[base : base + TILE, :], 0.0)
        edge = opening if piece == 0 else closing if piece == final else jnp.zeros_like(opening)
        high = jnp.concatenate([interior, edge], axis=0).astype(BF16)
        low = (jnp.concatenate([interior, edge], axis=0) - high.astype(F32)).astype(BF16)
        pieces.append(jnp.concatenate([high, low], axis=0))
    left = jnp.concatenate(pieces, axis=1)
    both = jnp.dot(left, jnp.concatenate([ref[...] for ref in split_refs], axis=1), preferred_element_type=F32)
    ends = slack[final:, :]
    scalars = jnp.where(
        sub == SQUARE_LAST,
        tail * ends,
        jnp.where(sub == LEAD_LAST, lead * ends, jnp.where(sub == SQUARE_FIRST, begin * slack[0:1, :], 0.0)),
    )
    scalars = jnp.broadcast_to(jnp.sum(scalars, axis=1, keepdims=True), (TILE, width))
    wide_sub = lax.broadcasted_iota(jnp.int32, (TILE, width), 0)
    half = 2 * TILE
    for place, ref in enumerate((own_ref, other_ref)):
        block = both[:, place * 2 * width : (place + 1) * 2 * width]
        sums = block[0:half, 0:width] + block[0:half, width : 2 * width] + block[half : 2 * half, 0:width]
        ref[...] = jnp.where(
            wide_sub == BACK,
            jnp.sum(sums[0:TILE, :], axis=0, keepdims=True),
            jnp.where(wide_sub <= TAIL_FIRST, sums[TILE:half, :], scalars),
        )
    edge_ref[...] = jnp.where(sub == 0, slack[0:1, :], ends)


def finish_kernel(scale_back, local, row_count, turns, *refs):
    messages = refs[:row_count]
    proj_ref, edge_ref, aux_ref, blend_ref, next_ref, out_ref = refs[row_count:]
    row = lax.axis_index("row")
    own_rows, width = proj_ref.shape[0], blend_ref.shape[1]
    group = LANES // local

    def own_lanes(x):
        mine = x[:, 0:LANES]
        for start in range(1, width // LANES):
            mine = jnp.where(row // group == start, x[:, start * LANES : (start + 1) * LANES], mine)
        return pltpu.roll(mine, (LANES - row % group * local) % LANES, 1)

    def by_block(received):
        blocks = []
        for block in range(row_count):
            mine = received[0]
            for turn in range(1, row_count):
                mine = jnp.where(lax.bitwise_xor(row, turn) == block, received[turn], mine)
            blocks.append(mine)
        return blocks

    received = [messages[turns.index(turn)][...] for turn in range(row_count)]
    scalars = by_block([m[:, 0:LANES] for m in received])
    vectors = by_block([own_lanes(m) for m in received])
    total = tree(b[BACK : BACK + 1, :] for b in vectors)
    ones = jnp.ones((1, LANES), F32)
    zeros = jnp.zeros((1, LANES), F32)
    tail_last, lead_last, tail_first = ones, zeros, ones
    for block in range(row_count - 1):
        this, that = scalars[block], scalars[block + 1]
        lead = this[LEAD_LAST : LEAD_LAST + 1, :]
        norm = jnp.sqrt(this[SQUARE_LAST : SQUARE_LAST + 1, :] + that[SQUARE_FIRST : SQUARE_FIRST + 1, :])
        inside = norm <= lead
        killed = norm <= -lead
        safe = jnp.where(norm > 0, norm, 1.0)
        middle = 0.5 * (lead + norm)
        factor = jnp.where(inside, 1.0, jnp.where(killed, 0.0, middle / safe))
        new = jnp.where(inside, lead, jnp.where(killed, 0.0, middle))
        tails = vectors[block][TAIL_LAST : TAIL_LAST + 1, :] + vectors[block + 1][TAIL_FIRST : TAIL_FIRST + 1, :]
        total = total + ((factor - 1.0) * tails + (new - lead) * vectors[block][HEAD_LAST : HEAD_LAST + 1, :])
        tail_last = jnp.where(row == block, factor, tail_last)
        lead_last = jnp.where(row == block, new, lead_last)
        tail_first = jnp.where(row == block + 1, factor, tail_first)
    next_ref[...] = (own_lanes(blend_ref[...]) - scale_back * total)[:, 0:local]
    final = own_rows - 1
    begin, end = edge_ref[0:1, :], edge_ref[1:2, :]
    ahead = jnp.where(aux_ref[FIRST, 0:1, :] > 0, tail_first * begin, proj_ref[0:1, :])
    closing = jnp.where(aux_ref[HEAD, final : final + 1, :] > 0, lead_last, tail_last * end)
    closing = jnp.where(aux_ref[LAST, final : final + 1, :] > 0, closing, proj_ref[final : final + 1, :])
    sub = lax.broadcasted_iota(jnp.int32, (own_rows, LANES), 0)
    out_ref[...] = jnp.where(sub == 0, ahead, jnp.where(sub == final, closing, proj_ref[...]))


def exchange(x, axis, turns):
    count = lax.axis_size(axis)
    return [lax.ppermute(x, axis, [(i, i ^ turn) for i in range(count)]) for turn in turns]


def exchange_rows(x):
    rows, cols = lax.axis_size("row"), lax.axis_size("col")
    return [
        lax.ppermute(x, ("row", "col"), [(r * cols + c, (r ^ turn) * cols + (c ^ 1)) for r in range(rows) for c in range(cols)])
        for turn in range(1, rows)
    ]


def merge_kernel(own_ref, far_ref, near_ref, out_ref):
    fetched = lax.bitwise_and(lax.axis_index("col"), 1) == 1
    out_ref[...] = near_ref[...] + jnp.where(fetched, far_ref[...], own_ref[...])


def reduce_chips(x, count):
    terms, bit = [x], 2
    while bit < count:
        x = tree(terms)
        if 2 * bit < count:
            far = lax.ppermute(x, "col", [(i, i ^ (3 * bit if i % 2 else bit)) for i in range(count)])
            near = lax.ppermute(x, "col", [(i, i ^ (2 * bit if i % 2 else bit)) for i in range(count)])
            x = pl.pallas_call(
                merge_kernel,
                name="merge",
                in_specs=[vmem()] * 3,
                out_specs=vmem(),
                out_shape=jax.ShapeDtypeStruct(x.shape, F32),
                compiler_params=params(),
            )(x, far, near)
            terms = [x, *exchange(x, "col", [1])]
        else:
            terms = [x, *exchange(x, "col", [bit])]
        bit *= 4
    return terms


def body(iterates, residuals, operator, target, cone_id):
    row_count = lax.axis_size("row")
    col_count = lax.axis_size("col")
    row_block, width = operator.shape
    hist, local = iterates.shape[0] - 1, iterates.shape[1]
    all_rows = row_block * row_count
    scale_back = math.sqrt(local * row_count * col_count / all_rows)
    wide, _, rows = dims(hist, local)
    own_rows = row_block // LANES

    (other,) = exchange(operator, "col", [1])
    message = pl.pallas_call(
        functools.partial(pack_kernel, hist, local),
        name="pack",
        in_specs=[pl.BlockSpec(memory_space=pltpu.HBM)] * 2,
        out_specs=vmem(),
        out_shape=jax.ShapeDtypeStruct((row_count * col_count * rows, LANES), F32),
        scratch_shapes=[
            pltpu.VMEM((hist + 1, local), F32),
            pltpu.VMEM((hist + 1, local), F32),
            pltpu.VMEM((wide, LANES), F32),
            pltpu.VMEM((-(-hist // TILE) * LANES, local), F32),
            pltpu.SemaphoreType.DMA((2,)),
        ],
        cost_estimate=pl.CostEstimate(flops=10**10, bytes_accessed=4 * 10**7, transcendentals=0),
        compiler_params=params(),
    )(hbm(iterates), hbm(residuals))
    received = lax.all_to_all(message, ("col", "row"), 0, 0, tiled=True)

    *halves, part, blended = pl.pallas_call(
        functools.partial(image_kernel, hist, local, row_count, min(512, row_block)),
        name="image",
        in_specs=[vmem()] * 3,
        out_specs=[vmem()] * 6,
        out_shape=[
            *[jax.ShapeDtypeStruct((row_block, width), BF16)] * 4,
            jax.ShapeDtypeStruct((own_rows, LANES), F32),
            jax.ShapeDtypeStruct((1, width), F32),
        ],
        scratch_shapes=[
            pltpu.VMEM((width // LANES, wide, LANES), F32),
            pltpu.VMEM((width // LANES, wide, LANES), F32),
            pltpu.VMEM(((hist + 1) * own_rows, LANES), F32),
        ],
        compiler_params=params(8 * operator.size),
    )(received, operator, other)

    aux = pl.pallas_call(
        functools.partial(mask_kernel, row_count),
        name="masks",
        in_specs=[vmem()] * 3,
        out_specs=vmem(),
        out_shape=jax.ShapeDtypeStruct((AUX, own_rows, LANES), F32),
        compiler_params=params(),
    )(cone_id.reshape(-1, LANES), target.reshape(-1, LANES), blended)

    parts = reduce_chips(part, col_count)
    projected, edge, own, other = pl.pallas_call(
        functools.partial(cone_kernel, len(parts)),
        name="cones",
        in_specs=[vmem()] * (len(parts) + 5),
        out_specs=[vmem()] * 4,
        out_shape=[
            jax.ShapeDtypeStruct((own_rows, LANES), F32),
            jax.ShapeDtypeStruct((TILE, LANES), F32),
            jax.ShapeDtypeStruct((TILE, width), F32),
            jax.ShapeDtypeStruct((TILE, width), F32),
        ],
        compiler_params=params(8 * operator.size),
    )(*parts, aux, *halves)

    turns = [0, 1, *range(3, row_count), 2]
    messages = [own, *exchange_rows(other)]
    next_point, projected = pl.pallas_call(
        functools.partial(finish_kernel, scale_back, local, row_count, turns),
        name="finish",
        in_specs=[vmem()] * (row_count + 4),
        out_specs=[vmem()] * 2,
        out_shape=[jax.ShapeDtypeStruct((1, local), F32), jax.ShapeDtypeStruct((own_rows, LANES), F32)],
        compiler_params=params(),
    )(*[messages[turn] for turn in turns], projected, edge, aux, blended)
    return (next_point.reshape(local), projected.reshape(row_block))


def solution(mesh):
    return jax.shard_map(
        body,
        mesh=mesh,
        in_specs=(P(None, ("col", "row")), P(None, ("col", "row")), P("row", "col"), P(), P()),
        out_specs=(P(("col", "row")), P("row")),
        check_vma=False,
    )
```

```python
import functools
import math

import jax
import jax.numpy as jnp
from jax import lax
from jax.experimental import pallas as pl
from jax.experimental.pallas import tpu as pltpu
from jax.sharding import PartitionSpec as P

LANES = 128
TILE = 8
BF16 = jnp.bfloat16
F32 = jnp.float32
SMALL = 8 * 1024 * 1024
SHIFTS = (1, 2, 3, 4, 8, 12)
LEVEL = 3
NT = (((1,), (1,)), ((), ()))
TARGET, HEAD, FIRST, LAST, UPWARD, DOWNWARD = 0, 1, 2, 3, 4, 4 + len(SHIFTS)
AUX = 4 + 2 * len(SHIFTS)
BACK, TAIL_LAST, HEAD_LAST, TAIL_FIRST, SQUARE_LAST, LEAD_LAST, SQUARE_FIRST = range(7)


def params(blocks=0):
    return pltpu.CompilerParams(vmem_limit_bytes=SMALL + blocks)


def vmem():
    return pl.BlockSpec(memory_space=pltpu.VMEM)


def hbm(x):
    return pltpu.with_memory_space_constraint(x, pltpu.HBM)


def tree(terms):
    terms = list(terms)
    while len(terms) > 1:
        terms = [a + b for a, b in zip(terms[::2], terms[1::2])]
    return terms[0]


def split(x):
    high = x.astype(BF16)
    return high, (x - high.astype(F32)).astype(BF16)


def shifted(x, step):
    rows, lanes = x.shape
    lane = lax.broadcasted_iota(jnp.int32, x.shape, 1)
    turned = pltpu.roll(x, step % lanes, 1)
    carried = pltpu.roll(turned, (1 if step > 0 else -1) % rows, 0)
    return jnp.where(lane < step if step > 0 else lane >= lanes + step, carried, turned)


def dims(hist, local):
    wide = -(-(hist + 1) // 16) * 16
    return wide, LANES // local, wide * local // LANES


def pack_kernel(hist, local, x_any, f_any, out_ref, x_ref, f_ref, dirs_ref, diff_ref, sems):
    wide, group, rows = dims(hist, local)
    pieces = -(-hist // TILE)
    copies = [pltpu.make_async_copy(a, b, sems.at[i]) for i, (a, b) in enumerate(((x_any, x_ref), (f_any, f_ref)))]
    for copy in copies:
        copy.start()
    dirs_ref[...] = jnp.zeros_like(dirs_ref)
    diff_ref[...] = jnp.zeros_like(diff_ref)
    for copy in copies:
        copy.wait()
    delta_f = f_ref[1 : hist + 1, :] - f_ref[0:hist, :]
    delta_x = x_ref[1 : hist + 1, :] - x_ref[0:hist, :]
    last_f = f_ref[hist : hist + 1, :]
    for piece in range(pieces):
        base = piece * (LANES + TILE * (hist + 1))
        diff_ref[base : base + hist, :] = delta_f
        diff_ref[base + hist : base + hist + 1, :] = last_f
    dirs_ref[0:hist, 0:local] = delta_x + delta_f
    dirs_ref[hist : hist + 1, 0:local] = x_ref[hist : hist + 1, :] + last_f
    gram = lax.dot_general(diff_ref[0:wide, :], diff_ref[...], NT, precision=lax.Precision.HIGHEST, preferred_element_type=F32)
    sub = lax.broadcasted_iota(jnp.int32, (TILE, LANES), 0)
    flat = jnp.zeros((TILE, LANES), F32)
    for piece in range(pieces):
        block = gram[piece * TILE : (piece + 1) * TILE, piece * LANES : (piece + 1) * LANES]
        block = jnp.where(sub < hist - piece * TILE, block, 0.0)
        flat = flat + pltpu.roll(block, 0, 1, stride=hist + 1, stride_axis=0)
    message = dirs_ref[pl.ds(0, rows, stride=group), :]
    for place in range(1, group):
        message = message + pltpu.roll(dirs_ref[pl.ds(place, rows, stride=group), :], place * local, 1)
    sub = lax.broadcasted_iota(jnp.int32, message.shape, 0)
    message = jnp.where(sub == rows - 1, jnp.sum(flat, axis=0, keepdims=True), message)
    message = jnp.concatenate([message] * (TILE // rows), axis=0)
    for start in range(0, out_ref.shape[0], TILE):
        out_ref[start : start + TILE, :] = message


def directions(hist, local, row_count, col, recv_ref, dirs_ref):
    wide, group, rows = dims(hist, local)
    mine = recv_ref[pl.ds(pl.multiple_of(col * (row_count * rows), TILE), row_count * rows), :]
    lane = lax.broadcasted_iota(jnp.int32, (rows, LANES), 1)
    width = row_count * local
    for start in range(0, width, LANES):
        for place in range(group):
            spread = jnp.zeros((rows, LANES), F32)
            for slot in range(group):
                block = start // local + slot
                moved = mine[block * rows : (block + 1) * rows, :]
                if slot != place:
                    moved = pltpu.roll(moved, (slot - place) * local % LANES, 1)
                spread = jnp.where(lane // local == slot, moved, spread)
            dirs_ref.at[start // LANES][pl.ds(place, rows, stride=group), :] = spread
    sub = lax.broadcasted_iota(jnp.int32, (wide, width), 0)
    dirs = jnp.concatenate([dirs_ref[i] for i in range(width // LANES)], axis=1)
    return jnp.where(sub <= hist, dirs, 0.0)


def left_operand(dirs):
    high, low = split(dirs)
    return jnp.concatenate(
        [jnp.concatenate([high, high], axis=1), jnp.concatenate([low, jnp.zeros_like(low)], axis=1)], axis=0
    )


def image_kernel(hist, local, row_count, chunk, recv_ref, *refs):
    oper_ref, other_ref, *split_refs, part_ref, blend_ref, dirs_ref, far_ref, img_ref = refs
    wide, _, rows = dims(hist, local)
    row_block, width = oper_ref.shape
    own_rows = row_block // LANES
    col = lax.axis_index("col")
    dirs = directions(hist, local, row_count, col, recv_ref, dirs_ref)
    left = left_operand(dirs)
    far = left_operand(directions(hist, local, row_count, lax.bitwise_xor(col, 1), recv_ref, far_ref))

    def multiply(left, high, low):
        both = lax.dot_general(left, jnp.concatenate([high, low], axis=1), NT, preferred_element_type=F32)
        return both[0:wide, :] + both[wide : 2 * wide, :]

    for start in range(0, row_block, chunk):
        own = split(oper_ref[start : start + chunk, :])
        other = split(other_ref[start : start + chunk, :])
        for ref, value in zip(split_refs, (*own, *other)):
            ref[start : start + chunk, :] = value
        image = multiply(left, *own) + multiply(far, *other)
        for piece in range(chunk // LANES):
            tile = image[:, piece * LANES : (piece + 1) * LANES]
            img_ref[pl.ds(start // LANES + piece, hist + 1, stride=own_rows), :] = tile[0 : hist + 1, :]

    flat = jnp.sum(recv_ref[pl.ds(rows - 1, recv_ref.shape[0] // rows, stride=rows), :], axis=0, keepdims=True)
    index = lax.broadcasted_iota(jnp.int32, (wide, LANES), 0)
    gram = jnp.where(index == 0, flat, 0.0)
    for k in range(1, hist):
        gram = jnp.where(index == k, pltpu.roll(flat, LANES - k * (hist + 1), 1), gram)
    cols = [jnp.broadcast_to(gram[:, j : j + 1], (wide, LANES)) for j in range(hist + 1)]

    def row_of(x, k):
        return jnp.broadcast_to(x[k : k + 1, :], (wide, LANES))

    trace = row_of(cols[0], 0)
    for k in range(1, hist):
        trace = trace + row_of(cols[k], k)
    ridge = 0.01 * (trace / hist)
    for k in range(hist):
        cols[k] = jnp.where(index == k, cols[k] + ridge, cols[k])
    for k in range(hist):
        inverse = 1.0 / row_of(cols[k], k)
        for j in range(k + 1, hist + 1):
            ratio = row_of(cols[j], k) * inverse
            cols[j] = jnp.where(index == k, ratio, cols[j] - cols[k] * ratio)
    weights = cols[hist]
    total = img_ref[hist * own_rows : (hist + 1) * own_rows, :]
    for k in range(hist):
        total = total - jnp.broadcast_to(weights[k : k + 1, :], (own_rows, LANES)) * img_ref[k * own_rows : (k + 1) * own_rows, :]
    part_ref[...] = total
    factors = jnp.where(index < hist, -weights, jnp.where(index == hist, 1.0, 0.0))
    for start in range(0, width, LANES):
        blend_ref[:, start : start + LANES] = jnp.sum(factors * dirs[:, start : start + LANES], axis=0, keepdims=True)


def mask_kernel(row_count, ids_ref, target_ref, blend_ref, aux_ref):
    own_rows = aux_ref.shape[1]
    row = lax.axis_index("row")
    first = row * own_rows
    ids = ids_ref[pl.ds(first, own_rows), :]
    before = ids_ref[pl.ds(jnp.maximum(first - 1, 0), 1), :]
    after = ids_ref[pl.ds(jnp.minimum(first + own_rows, ids_ref.shape[0] - 1), 1), :]
    before = jnp.broadcast_to(before[:, LANES - 1 :], (1, LANES))
    after = jnp.broadcast_to(after[:, 0:1], (1, LANES))
    opens = ((ids == before) & (row > 0)).astype(F32)
    aux_ref[TARGET] = target_ref[pl.ds(first, own_rows), :]
    aux_ref[FIRST] = opens
    aux_ref[LAST] = ((ids == after) & (row < row_count - 1)).astype(F32)
    for index, step in enumerate(SHIFTS):
        same = (shifted(ids, step) == ids).astype(F32)
        aux_ref[UPWARD + index] = same
        aux_ref[DOWNWARD + index] = (shifted(ids, -step) == ids).astype(F32)
        if step == 1:
            aux_ref[HEAD] = (1.0 - same) * (1.0 - opens)


def products(left, high, low, scalars):
    width = high.shape[1]
    both = jnp.dot(left, jnp.concatenate([high, low], axis=1), preferred_element_type=F32)
    half = 2 * TILE
    sums = both[0:half, 0:width] + both[0:half, width : 2 * width] + both[half : 2 * half, 0:width]
    sub = lax.broadcasted_iota(jnp.int32, (TILE, width), 0)
    return jnp.where(
        sub == BACK,
        jnp.sum(sums[0:TILE, :], axis=0, keepdims=True),
        jnp.where(sub <= TAIL_FIRST, sums[TILE:half, :], scalars),
    )


def own_kernel(left_ref, high_ref, low_ref, scalar_ref, out_ref):
    out_ref[...] = products(left_ref[...], high_ref[...], low_ref[...], scalar_ref[...])


def cone_kernel(count, *refs):
    parts = refs[:count]
    aux_ref, high_ref, low_ref, proj_ref, edge_ref, left_ref, scalar_ref, out_ref = refs[count:]
    own_rows = proj_ref.shape[0]
    width = out_ref.shape[1]
    slack = aux_ref[TARGET] - tree(p[...] for p in parts)
    head, first, last = aux_ref[HEAD], aux_ref[FIRST], aux_ref[LAST]
    square = (1.0 - head) * slack * slack
    lead, ahead, behind = head * slack, square, square
    for level in range(0, len(SHIFTS), LEVEL):
        places = range(level, level + LEVEL)
        lead = lead + sum(aux_ref[UPWARD + i] * shifted(lead, SHIFTS[i]) for i in places)
        ahead = ahead + sum(aux_ref[UPWARD + i] * shifted(ahead, SHIFTS[i]) for i in places)
        behind = behind + sum(aux_ref[DOWNWARD + i] * shifted(behind, -SHIFTS[i]) for i in places)
    norm = jnp.sqrt(jnp.maximum(ahead + behind - square, 0.0))
    inside = norm <= lead
    killed = norm <= -lead
    safe = jnp.where(norm > 0, norm, 1.0)
    middle = 0.5 * (lead + norm)
    outside = jnp.where(head > 0, middle, middle * slack / safe)
    projected = jnp.where(inside, slack, jnp.where(killed, 0.0, outside))
    proj_ref[...] = projected
    correction = jnp.where(first + last > 0, 0.0, projected - slack)

    sub = lax.broadcasted_iota(jnp.int32, (TILE, LANES), 0)
    final = own_rows - 1
    begin = (first * slack)[0:1, :]
    tail = (last * (1.0 - head) * slack)[final:, :]
    lead = (last * head)[final:, :]
    closing = jnp.where(sub == TAIL_LAST, tail, jnp.where(sub == HEAD_LAST, lead, 0.0))
    opening = jnp.where(sub == TAIL_FIRST, begin, 0.0)
    pieces = []
    for piece in range(own_rows):
        base = piece // TILE * TILE
        interior = jnp.where(sub == piece % TILE, correction[base : base + TILE, :], 0.0)
        edge = opening if piece == 0 else closing if piece == final else jnp.zeros_like(opening)
        high = jnp.concatenate([interior, edge], axis=0).astype(BF16)
        low = (jnp.concatenate([interior, edge], axis=0) - high.astype(F32)).astype(BF16)
        pieces.append(jnp.concatenate([high, low], axis=0))
    left = jnp.concatenate(pieces, axis=1)
    ends = slack[final:, :]
    scalars = jnp.where(
        sub == SQUARE_LAST,
        tail * ends,
        jnp.where(sub == LEAD_LAST, lead * ends, jnp.where(sub == SQUARE_FIRST, begin * slack[0:1, :], 0.0)),
    )
    scalars = jnp.broadcast_to(jnp.sum(scalars, axis=1, keepdims=True), (TILE, width))
    left_ref[...] = left
    scalar_ref[...] = scalars
    out_ref[...] = products(left, high_ref[...], low_ref[...], scalars)
    edge_ref[...] = jnp.where(sub == 0, slack[0:1, :], ends)


def finish_kernel(scale_back, local, row_count, turns, *refs):
    messages = refs[:row_count]
    proj_ref, edge_ref, aux_ref, blend_ref, next_ref, out_ref = refs[row_count:]
    row = lax.axis_index("row")
    own_rows, width = proj_ref.shape[0], blend_ref.shape[1]
    group = LANES // local

    def own_lanes(x):
        mine = x[:, 0:LANES]
        for start in range(1, width // LANES):
            mine = jnp.where(row // group == start, x[:, start * LANES : (start + 1) * LANES], mine)
        return pltpu.roll(mine, (LANES - row % group * local) % LANES, 1)

    def by_block(received):
        blocks = []
        for block in range(row_count):
            mine = received[0]
            for turn in range(1, row_count):
                mine = jnp.where(lax.bitwise_xor(row, turn) == block, received[turn], mine)
            blocks.append(mine)
        return blocks

    received = [messages[turns.index(turn)][...] for turn in range(row_count)]
    scalars = by_block([m[:, 0:LANES] for m in received])
    vectors = by_block([own_lanes(m) for m in received])
    total = tree(b[BACK : BACK + 1, :] for b in vectors)
    ones = jnp.ones((1, LANES), F32)
    zeros = jnp.zeros((1, LANES), F32)
    tail_last, lead_last, tail_first = ones, zeros, ones
    for block in range(row_count - 1):
        this, that = scalars[block], scalars[block + 1]
        lead = this[LEAD_LAST : LEAD_LAST + 1, :]
        norm = jnp.sqrt(this[SQUARE_LAST : SQUARE_LAST + 1, :] + that[SQUARE_FIRST : SQUARE_FIRST + 1, :])
        inside = norm <= lead
        killed = norm <= -lead
        safe = jnp.where(norm > 0, norm, 1.0)
        middle = 0.5 * (lead + norm)
        factor = jnp.where(inside, 1.0, jnp.where(killed, 0.0, middle / safe))
        new = jnp.where(inside, lead, jnp.where(killed, 0.0, middle))
        tails = vectors[block][TAIL_LAST : TAIL_LAST + 1, :] + vectors[block + 1][TAIL_FIRST : TAIL_FIRST + 1, :]
        total = total + ((factor - 1.0) * tails + (new - lead) * vectors[block][HEAD_LAST : HEAD_LAST + 1, :])
        tail_last = jnp.where(row == block, factor, tail_last)
        lead_last = jnp.where(row == block, new, lead_last)
        tail_first = jnp.where(row == block + 1, factor, tail_first)
    next_ref[...] = (own_lanes(blend_ref[...]) - scale_back * total)[:, 0:local]
    final = own_rows - 1
    begin, end = edge_ref[0:1, :], edge_ref[1:2, :]
    ahead = jnp.where(aux_ref[FIRST, 0:1, :] > 0, tail_first * begin, proj_ref[0:1, :])
    closing = jnp.where(aux_ref[HEAD, final : final + 1, :] > 0, lead_last, tail_last * end)
    closing = jnp.where(aux_ref[LAST, final : final + 1, :] > 0, closing, proj_ref[final : final + 1, :])
    sub = lax.broadcasted_iota(jnp.int32, (own_rows, LANES), 0)
    out_ref[...] = jnp.where(sub == 0, ahead, jnp.where(sub == final, closing, proj_ref[...]))


def exchange(x, axis, turns):
    count = lax.axis_size(axis)
    return [lax.ppermute(x, axis, [(i, i ^ turn) for i in range(count)]) for turn in turns]


def exchange_rows(x):
    rows, cols = lax.axis_size("row"), lax.axis_size("col")
    return [
        lax.ppermute(x, ("row", "col"), [(r * cols + c, (r ^ turn) * cols + (c ^ 1)) for r in range(rows) for c in range(cols)])
        for turn in range(1, rows)
    ]


def merge_kernel(own_ref, far_ref, near_ref, out_ref):
    fetched = lax.bitwise_and(lax.axis_index("col"), 1) == 1
    out_ref[...] = near_ref[...] + jnp.where(fetched, far_ref[...], own_ref[...])


def reduce_chips(x, count):
    terms, bit = [x], 2
    while bit < count:
        x = tree(terms)
        if 2 * bit < count:
            far = lax.ppermute(x, "col", [(i, i ^ (3 * bit if i % 2 else bit)) for i in range(count)])
            near = lax.ppermute(x, "col", [(i, i ^ (2 * bit if i % 2 else bit)) for i in range(count)])
            x = pl.pallas_call(
                merge_kernel,
                name="merge",
                in_specs=[vmem()] * 3,
                out_specs=vmem(),
                out_shape=jax.ShapeDtypeStruct(x.shape, F32),
                compiler_params=params(),
            )(x, far, near)
            terms = [x, *exchange(x, "col", [1])]
        else:
            terms = [x, *exchange(x, "col", [bit])]
        bit *= 4
    return terms


def body(iterates, residuals, operator, target, cone_id):
    row_count = lax.axis_size("row")
    col_count = lax.axis_size("col")
    row_block, width = operator.shape
    hist, local = iterates.shape[0] - 1, iterates.shape[1]
    all_rows = row_block * row_count
    scale_back = math.sqrt(local * row_count * col_count / all_rows)
    wide, _, rows = dims(hist, local)
    own_rows = row_block // LANES

    (other,) = exchange(operator, "col", [1])
    message = pl.pallas_call(
        functools.partial(pack_kernel, hist, local),
        name="pack",
        in_specs=[pl.BlockSpec(memory_space=pltpu.HBM)] * 2,
        out_specs=vmem(),
        out_shape=jax.ShapeDtypeStruct((row_count * col_count * rows, LANES), F32),
        scratch_shapes=[
            pltpu.VMEM((hist + 1, local), F32),
            pltpu.VMEM((hist + 1, local), F32),
            pltpu.VMEM((wide, LANES), F32),
            pltpu.VMEM((-(-hist // TILE) * LANES, local), F32),
            pltpu.SemaphoreType.DMA((2,)),
        ],
        cost_estimate=pl.CostEstimate(flops=10**10, bytes_accessed=4 * 10**7, transcendentals=0),
        compiler_params=params(),
    )(hbm(iterates), hbm(residuals))
    received = lax.all_to_all(message, ("col", "row"), 0, 0, tiled=True)

    *halves, part, blended = pl.pallas_call(
        functools.partial(image_kernel, hist, local, row_count, min(512, row_block)),
        name="image",
        in_specs=[vmem()] * 3,
        out_specs=[vmem()] * 6,
        out_shape=[
            *[jax.ShapeDtypeStruct((row_block, width), BF16)] * 4,
            jax.ShapeDtypeStruct((own_rows, LANES), F32),
            jax.ShapeDtypeStruct((1, width), F32),
        ],
        scratch_shapes=[
            pltpu.VMEM((width // LANES, wide, LANES), F32),
            pltpu.VMEM((width // LANES, wide, LANES), F32),
            pltpu.VMEM(((hist + 1) * own_rows, LANES), F32),
        ],
        compiler_params=params(8 * operator.size),
    )(received, operator, other)

    aux = pl.pallas_call(
        functools.partial(mask_kernel, row_count),
        name="masks",
        in_specs=[vmem()] * 3,
        out_specs=vmem(),
        out_shape=jax.ShapeDtypeStruct((AUX, own_rows, LANES), F32),
        compiler_params=params(),
    )(cone_id.reshape(-1, LANES), target.reshape(-1, LANES), blended)

    parts = reduce_chips(part, col_count)
    projected, edge, left, scalars, other = pl.pallas_call(
        functools.partial(cone_kernel, len(parts)),
        name="cones",
        in_specs=[vmem()] * (len(parts) + 3),
        out_specs=[vmem()] * 5,
        out_shape=[
            jax.ShapeDtypeStruct((own_rows, LANES), F32),
            jax.ShapeDtypeStruct((TILE, LANES), F32),
            jax.ShapeDtypeStruct((4 * TILE, row_block), BF16),
            jax.ShapeDtypeStruct((TILE, width), F32),
            jax.ShapeDtypeStruct((TILE, width), F32),
        ],
        compiler_params=params(8 * operator.size),
    )(*parts, aux, *halves[2:])
    own = pl.pallas_call(
        own_kernel,
        name="own",
        in_specs=[vmem()] * 4,
        out_specs=vmem(),
        out_shape=jax.ShapeDtypeStruct((TILE, width), F32),
        compiler_params=params(8 * operator.size),
    )(left, *halves[:2], scalars)

    turns = [0, 1, *range(3, row_count), 2]
    messages = [own, *exchange_rows(other)]
    next_point, projected = pl.pallas_call(
        functools.partial(finish_kernel, scale_back, local, row_count, turns),
        name="finish",
        in_specs=[vmem()] * (row_count + 4),
        out_specs=[vmem()] * 2,
        out_shape=[jax.ShapeDtypeStruct((1, local), F32), jax.ShapeDtypeStruct((own_rows, LANES), F32)],
        compiler_params=params(),
    )(*[messages[turn] for turn in turns], projected, edge, aux, blended)
    return (next_point.reshape(local), projected.reshape(row_block))


def solution(mesh):
    return jax.shard_map(
        body,
        mesh=mesh,
        in_specs=(P(None, ("col", "row")), P(None, ("col", "row")), P("row", "col"), P(), P()),
        out_specs=(P(("col", "row")), P("row")),
        check_vma=False,
    )
```

```python
import functools
import math

import jax
import jax.numpy as jnp
from jax import lax
from jax.experimental import pallas as pl
from jax.experimental.pallas import tpu as pltpu
from jax.sharding import PartitionSpec as P

LANES = 128
TILE = 8
BF16 = jnp.bfloat16
F32 = jnp.float32
SMALL = 8 * 1024 * 1024
SHIFTS = (1, 2, 3, 4, 8, 12)
LEVEL = 3
NT = (((1,), (1,)), ((), ()))
TARGET, HEAD, FIRST, LAST, UPWARD, DOWNWARD = 0, 1, 2, 3, 4, 4 + len(SHIFTS)
AUX = 4 + 2 * len(SHIFTS)
BACK, TAIL_LAST, HEAD_LAST, TAIL_FIRST, SQUARE_LAST, LEAD_LAST, SQUARE_FIRST = range(7)


def params(blocks=0):
    return pltpu.CompilerParams(vmem_limit_bytes=SMALL + blocks)


def vmem():
    return pl.BlockSpec(memory_space=pltpu.VMEM)


def tree(terms):
    terms = list(terms)
    while len(terms) > 1:
        terms = [a + b for a, b in zip(terms[::2], terms[1::2])]
    return terms[0]


def split(x):
    high = x.astype(BF16)
    return high, (x - high.astype(F32)).astype(BF16)


def shifted(x, step):
    rows, lanes = x.shape
    lane = lax.broadcasted_iota(jnp.int32, x.shape, 1)
    turned = pltpu.roll(x, step % lanes, 1)
    carried = pltpu.roll(turned, (1 if step > 0 else -1) % rows, 0)
    return jnp.where(lane < step if step > 0 else lane >= lanes + step, carried, turned)


def dims(hist, local):
    wide = -(-(hist + 1) // 16) * 16
    return wide, LANES // local, wide * local // LANES


def token_kernel(out_ref):
    out_ref[...] = jnp.zeros_like(out_ref)


def pack_kernel(hist, local, token_ref, x_ref, f_ref, out_ref, dirs_ref, diff_ref):
    wide, group, rows = dims(hist, local)
    pieces = -(-hist // TILE)
    dirs_ref[...] = jnp.zeros_like(dirs_ref)
    diff_ref[...] = jnp.zeros_like(diff_ref)
    delta_f = f_ref[1 : hist + 1, :] - f_ref[0:hist, :]
    delta_x = x_ref[1 : hist + 1, :] - x_ref[0:hist, :]
    last_f = f_ref[hist : hist + 1, :]
    for piece in range(pieces):
        base = piece * (LANES + TILE * (hist + 1))
        diff_ref[base : base + hist, :] = delta_f
        diff_ref[base + hist : base + hist + 1, :] = last_f
    dirs_ref[0:hist, 0:local] = delta_x + delta_f
    dirs_ref[hist : hist + 1, 0:local] = x_ref[hist : hist + 1, :] + last_f
    gram = lax.dot_general(diff_ref[0:wide, :], diff_ref[...], NT, precision=lax.Precision.HIGHEST, preferred_element_type=F32)
    sub = lax.broadcasted_iota(jnp.int32, (TILE, LANES), 0)
    flat = jnp.zeros((TILE, LANES), F32)
    for piece in range(pieces):
        block = gram[piece * TILE : (piece + 1) * TILE, piece * LANES : (piece + 1) * LANES]
        block = jnp.where(sub < hist - piece * TILE, block, 0.0)
        flat = flat + pltpu.roll(block, 0, 1, stride=hist + 1, stride_axis=0)
    message = dirs_ref[pl.ds(0, rows, stride=group), :]
    for place in range(1, group):
        message = message + pltpu.roll(dirs_ref[pl.ds(place, rows, stride=group), :], place * local, 1)
    sub = lax.broadcasted_iota(jnp.int32, message.shape, 0)
    message = jnp.where(sub == rows - 1, jnp.sum(flat, axis=0, keepdims=True), message)
    message = jnp.concatenate([message] * (TILE // rows), axis=0)
    for start in range(0, out_ref.shape[0], TILE):
        out_ref[start : start + TILE, :] = message


def directions(hist, local, row_count, col, recv_ref, dirs_ref):
    wide, group, rows = dims(hist, local)
    mine = recv_ref[pl.ds(pl.multiple_of(col * (row_count * rows), TILE), row_count * rows), :]
    lane = lax.broadcasted_iota(jnp.int32, (rows, LANES), 1)
    width = row_count * local
    for start in range(0, width, LANES):
        for place in range(group):
            spread = jnp.zeros((rows, LANES), F32)
            for slot in range(group):
                block = start // local + slot
                moved = mine[block * rows : (block + 1) * rows, :]
                if slot != place:
                    moved = pltpu.roll(moved, (slot - place) * local % LANES, 1)
                spread = jnp.where(lane // local == slot, moved, spread)
            dirs_ref.at[start // LANES][pl.ds(place, rows, stride=group), :] = spread
    sub = lax.broadcasted_iota(jnp.int32, (wide, width), 0)
    dirs = jnp.concatenate([dirs_ref[i] for i in range(width // LANES)], axis=1)
    return jnp.where(sub <= hist, dirs, 0.0)


def left_operand(dirs):
    high, low = split(dirs)
    return jnp.concatenate(
        [jnp.concatenate([high, high], axis=1), jnp.concatenate([low, jnp.zeros_like(low)], axis=1)], axis=0
    )


def image_kernel(hist, local, row_count, chunk, recv_ref, *refs):
    oper_ref, other_ref, *split_refs, part_ref, blend_ref, dirs_ref, far_ref, img_ref = refs
    wide, _, rows = dims(hist, local)
    row_block, width = oper_ref.shape
    own_rows = row_block // LANES
    col = lax.axis_index("col")
    dirs = directions(hist, local, row_count, col, recv_ref, dirs_ref)
    left = left_operand(dirs)
    far = left_operand(directions(hist, local, row_count, lax.bitwise_xor(col, 1), recv_ref, far_ref))

    def multiply(left, high, low):
        both = lax.dot_general(left, jnp.concatenate([high, low], axis=1), NT, preferred_element_type=F32)
        return both[0:wide, :] + both[wide : 2 * wide, :]

    for start in range(0, row_block, chunk):
        own = split(oper_ref[start : start + chunk, :])
        other = split(other_ref[start : start + chunk, :])
        for ref, value in zip(split_refs, (*own, *other)):
            ref[start : start + chunk, :] = value
        image = multiply(left, *own) + multiply(far, *other)
        for piece in range(chunk // LANES):
            tile = image[:, piece * LANES : (piece + 1) * LANES]
            img_ref[pl.ds(start // LANES + piece, hist + 1, stride=own_rows), :] = tile[0 : hist + 1, :]

    flat = jnp.sum(recv_ref[pl.ds(rows - 1, recv_ref.shape[0] // rows, stride=rows), :], axis=0, keepdims=True)
    index = lax.broadcasted_iota(jnp.int32, (wide, LANES), 0)
    gram = jnp.where(index == 0, flat, 0.0)
    for k in range(1, hist):
        gram = jnp.where(index == k, pltpu.roll(flat, LANES - k * (hist + 1), 1), gram)
    cols = [jnp.broadcast_to(gram[:, j : j + 1], (wide, LANES)) for j in range(hist + 1)]

    def row_of(x, k):
        return jnp.broadcast_to(x[k : k + 1, :], (wide, LANES))

    trace = row_of(cols[0], 0)
    for k in range(1, hist):
        trace = trace + row_of(cols[k], k)
    ridge = 0.01 * (trace / hist)
    for k in range(hist):
        cols[k] = jnp.where(index == k, cols[k] + ridge, cols[k])
    for k in range(hist):
        inverse = 1.0 / row_of(cols[k], k)
        for j in range(k + 1, hist + 1):
            ratio = row_of(cols[j], k) * inverse
            cols[j] = jnp.where(index == k, ratio, cols[j] - cols[k] * ratio)
    weights = cols[hist]
    total = img_ref[hist * own_rows : (hist + 1) * own_rows, :]
    for k in range(hist):
        total = total - jnp.broadcast_to(weights[k : k + 1, :], (own_rows, LANES)) * img_ref[k * own_rows : (k + 1) * own_rows, :]
    part_ref[...] = total
    factors = jnp.where(index < hist, -weights, jnp.where(index == hist, 1.0, 0.0))
    for start in range(0, width, LANES):
        blend_ref[:, start : start + LANES] = jnp.sum(factors * dirs[:, start : start + LANES], axis=0, keepdims=True)


def mask_kernel(row_count, ids_ref, target_ref, blend_ref, aux_ref):
    own_rows = aux_ref.shape[1]
    row = lax.axis_index("row")
    first = row * own_rows
    ids = ids_ref[pl.ds(first, own_rows), :]
    before = ids_ref[pl.ds(jnp.maximum(first - 1, 0), 1), :]
    after = ids_ref[pl.ds(jnp.minimum(first + own_rows, ids_ref.shape[0] - 1), 1), :]
    before = jnp.broadcast_to(before[:, LANES - 1 :], (1, LANES))
    after = jnp.broadcast_to(after[:, 0:1], (1, LANES))
    opens = ((ids == before) & (row > 0)).astype(F32)
    aux_ref[TARGET] = target_ref[pl.ds(first, own_rows), :]
    aux_ref[FIRST] = opens
    aux_ref[LAST] = ((ids == after) & (row < row_count - 1)).astype(F32)
    for index, step in enumerate(SHIFTS):
        same = (shifted(ids, step) == ids).astype(F32)
        aux_ref[UPWARD + index] = same
        aux_ref[DOWNWARD + index] = (shifted(ids, -step) == ids).astype(F32)
        if step == 1:
            aux_ref[HEAD] = (1.0 - same) * (1.0 - opens)


def products(left, high, low, scalars):
    width = high.shape[1]
    both = jnp.dot(left, jnp.concatenate([high, low], axis=1), preferred_element_type=F32)
    half = 2 * TILE
    sums = both[0:half, 0:width] + both[0:half, width : 2 * width] + both[half : 2 * half, 0:width]
    sub = lax.broadcasted_iota(jnp.int32, (TILE, width), 0)
    return jnp.where(
        sub == BACK,
        jnp.sum(sums[0:TILE, :], axis=0, keepdims=True),
        jnp.where(sub <= TAIL_FIRST, sums[TILE:half, :], scalars),
    )


def own_kernel(left_ref, high_ref, low_ref, scalar_ref, out_ref):
    out_ref[...] = products(left_ref[...], high_ref[...], low_ref[...], scalar_ref[...])


def cone_kernel(count, *refs):
    parts = refs[:count]
    aux_ref, high_ref, low_ref, proj_ref, edge_ref, left_ref, scalar_ref, out_ref = refs[count:]
    own_rows = proj_ref.shape[0]
    width = out_ref.shape[1]
    slack = aux_ref[TARGET] - tree(p[...] for p in parts)
    head, first, last = aux_ref[HEAD], aux_ref[FIRST], aux_ref[LAST]
    square = (1.0 - head) * slack * slack
    lead, ahead, behind = head * slack, square, square
    for level in range(0, len(SHIFTS), LEVEL):
        places = range(level, level + LEVEL)
        lead = lead + sum(aux_ref[UPWARD + i] * shifted(lead, SHIFTS[i]) for i in places)
        ahead = ahead + sum(aux_ref[UPWARD + i] * shifted(ahead, SHIFTS[i]) for i in places)
        behind = behind + sum(aux_ref[DOWNWARD + i] * shifted(behind, -SHIFTS[i]) for i in places)
    norm = jnp.sqrt(jnp.maximum(ahead + behind - square, 0.0))
    inside = norm <= lead
    killed = norm <= -lead
    safe = jnp.where(norm > 0, norm, 1.0)
    middle = 0.5 * (lead + norm)
    outside = jnp.where(head > 0, middle, middle * slack / safe)
    projected = jnp.where(inside, slack, jnp.where(killed, 0.0, outside))
    proj_ref[...] = projected
    correction = jnp.where(first + last > 0, 0.0, projected - slack)

    sub = lax.broadcasted_iota(jnp.int32, (TILE, LANES), 0)
    final = own_rows - 1
    begin = (first * slack)[0:1, :]
    tail = (last * (1.0 - head) * slack)[final:, :]
    lead = (last * head)[final:, :]
    closing = jnp.where(sub == TAIL_LAST, tail, jnp.where(sub == HEAD_LAST, lead, 0.0))
    opening = jnp.where(sub == TAIL_FIRST, begin, 0.0)
    pieces = []
    for piece in range(own_rows):
        base = piece // TILE * TILE
        interior = jnp.where(sub == piece % TILE, correction[base : base + TILE, :], 0.0)
        edge = opening if piece == 0 else closing if piece == final else jnp.zeros_like(opening)
        high = jnp.concatenate([interior, edge], axis=0).astype(BF16)
        low = (jnp.concatenate([interior, edge], axis=0) - high.astype(F32)).astype(BF16)
        pieces.append(jnp.concatenate([high, low], axis=0))
    left = jnp.concatenate(pieces, axis=1)
    ends = slack[final:, :]
    scalars = jnp.where(
        sub == SQUARE_LAST,
        tail * ends,
        jnp.where(sub == LEAD_LAST, lead * ends, jnp.where(sub == SQUARE_FIRST, begin * slack[0:1, :], 0.0)),
    )
    scalars = jnp.broadcast_to(jnp.sum(scalars, axis=1, keepdims=True), (TILE, width))
    left_ref[...] = left
    scalar_ref[...] = scalars
    out_ref[...] = products(left, high_ref[...], low_ref[...], scalars)
    edge_ref[...] = jnp.where(sub == 0, slack[0:1, :], ends)


def finish_kernel(scale_back, local, row_count, turns, *refs):
    messages = refs[:row_count]
    proj_ref, edge_ref, aux_ref, blend_ref, next_ref, out_ref = refs[row_count:]
    row = lax.axis_index("row")
    own_rows, width = proj_ref.shape[0], blend_ref.shape[1]
    group = LANES // local

    def own_lanes(x):
        mine = x[:, 0:LANES]
        for start in range(1, width // LANES):
            mine = jnp.where(row // group == start, x[:, start * LANES : (start + 1) * LANES], mine)
        return pltpu.roll(mine, (LANES - row % group * local) % LANES, 1)

    def by_block(received):
        blocks = []
        for block in range(row_count):
            mine = received[0]
            for turn in range(1, row_count):
                mine = jnp.where(lax.bitwise_xor(row, turn) == block, received[turn], mine)
            blocks.append(mine)
        return blocks

    received = [messages[turns.index(turn)][...] for turn in range(row_count)]
    scalars = by_block([m[:, 0:LANES] for m in received])
    vectors = by_block([own_lanes(m) for m in received])
    total = tree(b[BACK : BACK + 1, :] for b in vectors)
    ones = jnp.ones((1, LANES), F32)
    zeros = jnp.zeros((1, LANES), F32)
    tail_last, lead_last, tail_first = ones, zeros, ones
    for block in range(row_count - 1):
        this, that = scalars[block], scalars[block + 1]
        lead = this[LEAD_LAST : LEAD_LAST + 1, :]
        norm = jnp.sqrt(this[SQUARE_LAST : SQUARE_LAST + 1, :] + that[SQUARE_FIRST : SQUARE_FIRST + 1, :])
        inside = norm <= lead
        killed = norm <= -lead
        safe = jnp.where(norm > 0, norm, 1.0)
        middle = 0.5 * (lead + norm)
        factor = jnp.where(inside, 1.0, jnp.where(killed, 0.0, middle / safe))
        new = jnp.where(inside, lead, jnp.where(killed, 0.0, middle))
        tails = vectors[block][TAIL_LAST : TAIL_LAST + 1, :] + vectors[block + 1][TAIL_FIRST : TAIL_FIRST + 1, :]
        total = total + ((factor - 1.0) * tails + (new - lead) * vectors[block][HEAD_LAST : HEAD_LAST + 1, :])
        tail_last = jnp.where(row == block, factor, tail_last)
        lead_last = jnp.where(row == block, new, lead_last)
        tail_first = jnp.where(row == block + 1, factor, tail_first)
    next_ref[...] = (own_lanes(blend_ref[...]) - scale_back * total)[:, 0:local]
    final = own_rows - 1
    begin, end = edge_ref[0:1, :], edge_ref[1:2, :]
    ahead = jnp.where(aux_ref[FIRST, 0:1, :] > 0, tail_first * begin, proj_ref[0:1, :])
    closing = jnp.where(aux_ref[HEAD, final : final + 1, :] > 0, lead_last, tail_last * end)
    closing = jnp.where(aux_ref[LAST, final : final + 1, :] > 0, closing, proj_ref[final : final + 1, :])
    sub = lax.broadcasted_iota(jnp.int32, (own_rows, LANES), 0)
    out_ref[...] = jnp.where(sub == 0, ahead, jnp.where(sub == final, closing, proj_ref[...]))


def exchange(x, axis, turns):
    count = lax.axis_size(axis)
    return [lax.ppermute(x, axis, [(i, i ^ turn) for i in range(count)]) for turn in turns]


def exchange_rows(x):
    rows, cols = lax.axis_size("row"), lax.axis_size("col")
    return [
        lax.ppermute(x, ("row", "col"), [(r * cols + c, (r ^ turn) * cols + (c ^ 1)) for r in range(rows) for c in range(cols)])
        for turn in range(1, rows)
    ]


def merge_kernel(own_ref, far_ref, near_ref, out_ref):
    fetched = lax.bitwise_and(lax.axis_index("col"), 1) == 1
    out_ref[...] = near_ref[...] + jnp.where(fetched, far_ref[...], own_ref[...])


def reduce_chips(x, count):
    terms, bit = [x], 2
    while bit < count:
        x = tree(terms)
        if 2 * bit < count:
            far = lax.ppermute(x, "col", [(i, i ^ (3 * bit if i % 2 else bit)) for i in range(count)])
            near = lax.ppermute(x, "col", [(i, i ^ (2 * bit if i % 2 else bit)) for i in range(count)])
            x = pl.pallas_call(
                merge_kernel,
                name="merge",
                in_specs=[vmem()] * 3,
                out_specs=vmem(),
                out_shape=jax.ShapeDtypeStruct(x.shape, F32),
                compiler_params=params(),
            )(x, far, near)
            terms = [x, *exchange(x, "col", [1])]
        else:
            terms = [x, *exchange(x, "col", [bit])]
        bit *= 4
    return terms


def body(iterates, residuals, operator, target, cone_id):
    row_count = lax.axis_size("row")
    col_count = lax.axis_size("col")
    row_block, width = operator.shape
    hist, local = iterates.shape[0] - 1, iterates.shape[1]
    all_rows = row_block * row_count
    scale_back = math.sqrt(local * row_count * col_count / all_rows)
    wide, _, rows = dims(hist, local)
    own_rows = row_block // LANES

    (other,) = exchange(operator, "col", [1])
    token = pl.pallas_call(
        token_kernel,
        name="token",
        out_specs=vmem(),
        out_shape=jax.ShapeDtypeStruct((TILE, LANES), F32),
        cost_estimate=pl.CostEstimate(flops=10**10, bytes_accessed=4 * 10**7, transcendentals=0),
        compiler_params=params(),
    )()
    message = pl.pallas_call(
        functools.partial(pack_kernel, hist, local),
        name="pack",
        in_specs=[vmem()] * 3,
        out_specs=vmem(),
        out_shape=jax.ShapeDtypeStruct((row_count * col_count * rows, LANES), F32),
        scratch_shapes=[
            pltpu.VMEM((wide, LANES), F32),
            pltpu.VMEM((-(-hist // TILE) * LANES, local), F32),
        ],
        cost_estimate=pl.CostEstimate(flops=10**10, bytes_accessed=4 * 10**7, transcendentals=0),
        compiler_params=params(),
    )(token, iterates, residuals)
    received = lax.all_to_all(message, ("col", "row"), 0, 0, tiled=True)

    *halves, part, blended = pl.pallas_call(
        functools.partial(image_kernel, hist, local, row_count, min(512, row_block)),
        name="image",
        in_specs=[vmem()] * 3,
        out_specs=[vmem()] * 6,
        out_shape=[
            *[jax.ShapeDtypeStruct((row_block, width), BF16)] * 4,
            jax.ShapeDtypeStruct((own_rows, LANES), F32),
            jax.ShapeDtypeStruct((1, width), F32),
        ],
        scratch_shapes=[
            pltpu.VMEM((width // LANES, wide, LANES), F32),
            pltpu.VMEM((width // LANES, wide, LANES), F32),
            pltpu.VMEM(((hist + 1) * own_rows, LANES), F32),
        ],
        compiler_params=params(8 * operator.size),
    )(received, operator, other)

    aux = pl.pallas_call(
        functools.partial(mask_kernel, row_count),
        name="masks",
        in_specs=[vmem()] * 3,
        out_specs=vmem(),
        out_shape=jax.ShapeDtypeStruct((AUX, own_rows, LANES), F32),
        compiler_params=params(),
    )(cone_id.reshape(-1, LANES), target.reshape(-1, LANES), blended)

    parts = reduce_chips(part, col_count)
    projected, edge, left, scalars, other = pl.pallas_call(
        functools.partial(cone_kernel, len(parts)),
        name="cones",
        in_specs=[vmem()] * (len(parts) + 3),
        out_specs=[vmem()] * 5,
        out_shape=[
            jax.ShapeDtypeStruct((own_rows, LANES), F32),
            jax.ShapeDtypeStruct((TILE, LANES), F32),
            jax.ShapeDtypeStruct((4 * TILE, row_block), BF16),
            jax.ShapeDtypeStruct((TILE, width), F32),
            jax.ShapeDtypeStruct((TILE, width), F32),
        ],
        compiler_params=params(8 * operator.size),
    )(*parts, aux, *halves[2:])
    own = pl.pallas_call(
        own_kernel,
        name="own",
        in_specs=[vmem()] * 4,
        out_specs=vmem(),
        out_shape=jax.ShapeDtypeStruct((TILE, width), F32),
        compiler_params=params(8 * operator.size),
    )(left, *halves[:2], scalars)

    turns = [0, 1, *range(3, row_count), 2]
    messages = [own, *exchange_rows(other)]
    next_point, projected = pl.pallas_call(
        functools.partial(finish_kernel, scale_back, local, row_count, turns),
        name="finish",
        in_specs=[vmem()] * (row_count + 4),
        out_specs=[vmem()] * 2,
        out_shape=[jax.ShapeDtypeStruct((1, local), F32), jax.ShapeDtypeStruct((own_rows, LANES), F32)],
        compiler_params=params(),
    )(*[messages[turn] for turn in turns], projected, edge, aux, blended)
    return (next_point.reshape(local), projected.reshape(row_block))


def solution(mesh):
    return jax.shard_map(
        body,
        mesh=mesh,
        in_specs=(P(None, ("col", "row")), P(None, ("col", "row")), P("row", "col"), P(), P()),
        out_specs=(P(("col", "row")), P("row")),
        check_vma=False,
    )
```

```python
import functools
import math

import jax
import jax.numpy as jnp
from jax import lax
from jax.experimental import pallas as pl
from jax.experimental.pallas import tpu as pltpu
from jax.sharding import PartitionSpec as P

LANES = 128
TILE = 8
BF16 = jnp.bfloat16
F32 = jnp.float32
SMALL = 8 * 1024 * 1024
SHIFTS = (1, 2, 3, 4, 8, 12)
LEVEL = 3
NT = (((1,), (1,)), ((), ()))
TARGET, HEAD, FIRST, LAST, UPWARD, DOWNWARD = 0, 1, 2, 3, 4, 4 + len(SHIFTS)
AUX = 4 + 2 * len(SHIFTS)
BACK, TAIL_LAST, HEAD_LAST, TAIL_FIRST, SQUARE_LAST, LEAD_LAST, SQUARE_FIRST = range(7)


def params(blocks=0):
    return pltpu.CompilerParams(vmem_limit_bytes=SMALL + blocks)


def vmem():
    return pl.BlockSpec(memory_space=pltpu.VMEM)


def tree(terms):
    terms = list(terms)
    while len(terms) > 1:
        terms = [a + b for a, b in zip(terms[::2], terms[1::2])]
    return terms[0]


def split(x):
    high = x.astype(BF16)
    return high, (x - high.astype(F32)).astype(BF16)


def shifted(x, step):
    rows, lanes = x.shape
    lane = lax.broadcasted_iota(jnp.int32, x.shape, 1)
    turned = pltpu.roll(x, step % lanes, 1)
    carried = pltpu.roll(turned, (1 if step > 0 else -1) % rows, 0)
    return jnp.where(lane < step if step > 0 else lane >= lanes + step, carried, turned)


def dims(hist, local):
    wide = -(-(hist + 1) // 16) * 16
    return wide, LANES // local, wide * local // LANES


def token_kernel(out_ref):
    out_ref[...] = jnp.zeros_like(out_ref)


def pack_kernel(hist, local, token_ref, x_ref, f_ref, out_ref, dirs_ref, diff_ref):
    wide, group, rows = dims(hist, local)
    pieces = -(-hist // TILE)
    dirs_ref[...] = jnp.zeros_like(dirs_ref)
    diff_ref[...] = jnp.zeros_like(diff_ref)
    delta_f = f_ref[1 : hist + 1, :] - f_ref[0:hist, :]
    delta_x = x_ref[1 : hist + 1, :] - x_ref[0:hist, :]
    last_f = f_ref[hist : hist + 1, :]
    for piece in range(pieces):
        base = piece * (LANES + TILE * (hist + 1))
        diff_ref[base : base + hist, :] = delta_f
        diff_ref[base + hist : base + hist + 1, :] = last_f
    dirs_ref[0:hist, 0:local] = delta_x + delta_f
    dirs_ref[hist : hist + 1, 0:local] = x_ref[hist : hist + 1, :] + last_f
    gram = lax.dot_general(diff_ref[0:wide, :], diff_ref[...], NT, precision=lax.Precision.HIGHEST, preferred_element_type=F32)
    sub = lax.broadcasted_iota(jnp.int32, (TILE, LANES), 0)
    flat = jnp.zeros((TILE, LANES), F32)
    for piece in range(pieces):
        block = gram[piece * TILE : (piece + 1) * TILE, piece * LANES : (piece + 1) * LANES]
        block = jnp.where(sub < hist - piece * TILE, block, 0.0)
        flat = flat + pltpu.roll(block, 0, 1, stride=hist + 1, stride_axis=0)
    message = dirs_ref[pl.ds(0, rows, stride=group), :]
    for place in range(1, group):
        message = message + pltpu.roll(dirs_ref[pl.ds(place, rows, stride=group), :], place * local, 1)
    sub = lax.broadcasted_iota(jnp.int32, message.shape, 0)
    message = jnp.where(sub == rows - 1, jnp.sum(flat, axis=0, keepdims=True), message)
    message = jnp.concatenate([message] * (TILE // rows), axis=0)
    for start in range(0, out_ref.shape[0], TILE):
        out_ref[start : start + TILE, :] = message


def directions(hist, local, row_count, col, recv_ref, dirs_ref):
    wide, group, rows = dims(hist, local)
    mine = recv_ref[pl.ds(pl.multiple_of(col * (row_count * rows), TILE), row_count * rows), :]
    lane = lax.broadcasted_iota(jnp.int32, (rows, LANES), 1)
    width = row_count * local
    for start in range(0, width, LANES):
        for place in range(group):
            spread = jnp.zeros((rows, LANES), F32)
            for slot in range(group):
                block = start // local + slot
                moved = mine[block * rows : (block + 1) * rows, :]
                if slot != place:
                    moved = pltpu.roll(moved, (slot - place) * local % LANES, 1)
                spread = jnp.where(lane // local == slot, moved, spread)
            dirs_ref.at[start // LANES][pl.ds(place, rows, stride=group), :] = spread
    sub = lax.broadcasted_iota(jnp.int32, (wide, width), 0)
    dirs = jnp.concatenate([dirs_ref[i] for i in range(width // LANES)], axis=1)
    return jnp.where(sub <= hist, dirs, 0.0)


def left_operand(dirs):
    high, low = split(dirs)
    return jnp.concatenate(
        [jnp.concatenate([high, high], axis=1), jnp.concatenate([low, jnp.zeros_like(low)], axis=1)], axis=0
    )


def image_kernel(hist, local, row_count, chunk, recv_ref, *refs):
    oper_ref, other_ref, *split_refs, part_ref, blend_ref, dirs_ref, far_ref, img_ref = refs
    wide, _, rows = dims(hist, local)
    row_block, width = oper_ref.shape
    own_rows = row_block // LANES
    col = lax.axis_index("col")
    dirs = directions(hist, local, row_count, col, recv_ref, dirs_ref)
    left = left_operand(dirs)
    far = left_operand(directions(hist, local, row_count, lax.bitwise_xor(col, 1), recv_ref, far_ref))

    def multiply(left, high, low):
        both = lax.dot_general(left, jnp.concatenate([high, low], axis=1), NT, preferred_element_type=F32)
        return both[0:wide, :] + both[wide : 2 * wide, :]

    for start in range(0, row_block, chunk):
        own = split(oper_ref[start : start + chunk, :])
        other = split(other_ref[start : start + chunk, :])
        for ref, value in zip(split_refs, (*own, *other)):
            ref[start : start + chunk, :] = value
        image = multiply(left, *own) + multiply(far, *other)
        for piece in range(chunk // LANES):
            tile = image[:, piece * LANES : (piece + 1) * LANES]
            img_ref[pl.ds(start // LANES + piece, hist + 1, stride=own_rows), :] = tile[0 : hist + 1, :]

    flat = jnp.sum(recv_ref[pl.ds(rows - 1, recv_ref.shape[0] // rows, stride=rows), :], axis=0, keepdims=True)
    index = lax.broadcasted_iota(jnp.int32, (wide, LANES), 0)
    gram = jnp.where(index == 0, flat, 0.0)
    for k in range(1, hist):
        gram = jnp.where(index == k, pltpu.roll(flat, LANES - k * (hist + 1), 1), gram)
    cols = [jnp.broadcast_to(gram[:, j : j + 1], (wide, LANES)) for j in range(hist + 1)]

    def row_of(x, k):
        return jnp.broadcast_to(x[k : k + 1, :], (wide, LANES))

    trace = row_of(cols[0], 0)
    for k in range(1, hist):
        trace = trace + row_of(cols[k], k)
    ridge = 0.01 * (trace / hist)
    for k in range(hist):
        cols[k] = jnp.where(index == k, cols[k] + ridge, cols[k])
    for k in range(hist):
        inverse = 1.0 / row_of(cols[k], k)
        for j in range(k + 1, hist + 1):
            ratio = row_of(cols[j], k) * inverse
            cols[j] = jnp.where(index == k, ratio, cols[j] - cols[k] * ratio)
    weights = cols[hist]
    total = img_ref[hist * own_rows : (hist + 1) * own_rows, :]
    for k in range(hist):
        total = total - jnp.broadcast_to(weights[k : k + 1, :], (own_rows, LANES)) * img_ref[k * own_rows : (k + 1) * own_rows, :]
    part_ref[...] = total
    factors = jnp.where(index < hist, -weights, jnp.where(index == hist, 1.0, 0.0))
    for start in range(0, width, LANES):
        blend_ref[:, start : start + LANES] = jnp.sum(factors * dirs[:, start : start + LANES], axis=0, keepdims=True)


def mask_kernel(row_count, ids_ref, target_ref, blend_ref, aux_ref):
    own_rows = aux_ref.shape[1]
    row = lax.axis_index("row")
    first = row * own_rows
    ids = ids_ref[pl.ds(first, own_rows), :]
    before = ids_ref[pl.ds(jnp.maximum(first - 1, 0), 1), :]
    after = ids_ref[pl.ds(jnp.minimum(first + own_rows, ids_ref.shape[0] - 1), 1), :]
    before = jnp.broadcast_to(before[:, LANES - 1 :], (1, LANES))
    after = jnp.broadcast_to(after[:, 0:1], (1, LANES))
    opens = ((ids == before) & (row > 0)).astype(F32)
    aux_ref[TARGET] = target_ref[pl.ds(first, own_rows), :]
    aux_ref[FIRST] = opens
    aux_ref[LAST] = ((ids == after) & (row < row_count - 1)).astype(F32)
    for index, step in enumerate(SHIFTS):
        same = (shifted(ids, step) == ids).astype(F32)
        aux_ref[UPWARD + index] = same
        aux_ref[DOWNWARD + index] = (shifted(ids, -step) == ids).astype(F32)
        if step == 1:
            aux_ref[HEAD] = (1.0 - same) * (1.0 - opens)


def products(left, high, low, scalars):
    width = high.shape[1]
    both = jnp.dot(left, jnp.concatenate([high, low], axis=1), preferred_element_type=F32)
    half = 2 * TILE
    sums = both[0:half, 0:width] + both[0:half, width : 2 * width] + both[half : 2 * half, 0:width]
    sub = lax.broadcasted_iota(jnp.int32, (TILE, width), 0)
    return jnp.where(
        sub == BACK,
        jnp.sum(sums[0:TILE, :], axis=0, keepdims=True),
        jnp.where(sub <= TAIL_FIRST, sums[TILE:half, :], scalars),
    )


def own_kernel(left_ref, high_ref, low_ref, scalar_ref, out_ref):
    out_ref[...] = products(left_ref[...], high_ref[...], low_ref[...], scalar_ref[...])


def cone_kernel(count, *refs):
    parts = refs[:count]
    aux_ref, high_ref, low_ref, proj_ref, edge_ref, left_ref, scalar_ref, out_ref = refs[count:]
    own_rows = proj_ref.shape[0]
    width = out_ref.shape[1]
    slack = aux_ref[TARGET] - tree(p[...] for p in parts)
    head, first, last = aux_ref[HEAD], aux_ref[FIRST], aux_ref[LAST]
    square = (1.0 - head) * slack * slack
    lead, ahead, behind = head * slack, square, square
    for level in range(0, len(SHIFTS), LEVEL):
        places = range(level, level + LEVEL)
        lead = lead + sum(aux_ref[UPWARD + i] * shifted(lead, SHIFTS[i]) for i in places)
        ahead = ahead + sum(aux_ref[UPWARD + i] * shifted(ahead, SHIFTS[i]) for i in places)
        behind = behind + sum(aux_ref[DOWNWARD + i] * shifted(behind, -SHIFTS[i]) for i in places)
    norm = jnp.sqrt(jnp.maximum(ahead + behind - square, 0.0))
    inside = norm <= lead
    killed = norm <= -lead
    safe = jnp.where(norm > 0, norm, 1.0)
    middle = 0.5 * (lead + norm)
    outside = jnp.where(head > 0, middle, middle * slack / safe)
    projected = jnp.where(inside, slack, jnp.where(killed, 0.0, outside))
    proj_ref[...] = projected
    correction = jnp.where(first + last > 0, 0.0, projected - slack)

    sub = lax.broadcasted_iota(jnp.int32, (TILE, LANES), 0)
    final = own_rows - 1
    begin = (first * slack)[0:1, :]
    tail = (last * (1.0 - head) * slack)[final:, :]
    lead = (last * head)[final:, :]
    closing = jnp.where(sub == TAIL_LAST, tail, jnp.where(sub == HEAD_LAST, lead, 0.0))
    opening = jnp.where(sub == TAIL_FIRST, begin, 0.0)
    pieces = []
    for piece in range(own_rows):
        base = piece // TILE * TILE
        interior = jnp.where(sub == piece % TILE, correction[base : base + TILE, :], 0.0)
        edge = opening if piece == 0 else closing if piece == final else jnp.zeros_like(opening)
        high = jnp.concatenate([interior, edge], axis=0).astype(BF16)
        low = (jnp.concatenate([interior, edge], axis=0) - high.astype(F32)).astype(BF16)
        pieces.append(jnp.concatenate([high, low], axis=0))
    left = jnp.concatenate(pieces, axis=1)
    ends = slack[final:, :]
    scalars = jnp.where(
        sub == SQUARE_LAST,
        tail * ends,
        jnp.where(sub == LEAD_LAST, lead * ends, jnp.where(sub == SQUARE_FIRST, begin * slack[0:1, :], 0.0)),
    )
    scalars = jnp.broadcast_to(jnp.sum(scalars, axis=1, keepdims=True), (TILE, width))
    left_ref[...] = left
    scalar_ref[...] = scalars
    out_ref[...] = products(left, high_ref[...], low_ref[...], scalars)
    edge_ref[...] = jnp.where(sub == 0, slack[0:1, :], ends)


def finish_kernel(scale_back, local, row_count, turns, *refs):
    messages = refs[:row_count]
    proj_ref, edge_ref, aux_ref, blend_ref, next_ref, out_ref = refs[row_count:]
    row = lax.axis_index("row")
    own_rows, width = proj_ref.shape[0], blend_ref.shape[1]
    group = LANES // local

    def own_lanes(x):
        mine = x[:, 0:LANES]
        for start in range(1, width // LANES):
            mine = jnp.where(row // group == start, x[:, start * LANES : (start + 1) * LANES], mine)
        return pltpu.roll(mine, (LANES - row % group * local) % LANES, 1)

    def by_block(received):
        blocks = []
        for block in range(row_count):
            mine = received[0]
            for turn in range(1, row_count):
                mine = jnp.where(lax.bitwise_xor(row, turn) == block, received[turn], mine)
            blocks.append(mine)
        return blocks

    received = [messages[turns.index(turn)][...] for turn in range(row_count)]
    scalars = by_block([m[:, 0:LANES] for m in received])
    vectors = by_block([own_lanes(m) for m in received])
    total = tree(b[BACK : BACK + 1, :] for b in vectors)
    ones = jnp.ones((1, LANES), F32)
    zeros = jnp.zeros((1, LANES), F32)
    tail_last, lead_last, tail_first = ones, zeros, ones
    for block in range(row_count - 1):
        this, that = scalars[block], scalars[block + 1]
        lead = this[LEAD_LAST : LEAD_LAST + 1, :]
        norm = jnp.sqrt(this[SQUARE_LAST : SQUARE_LAST + 1, :] + that[SQUARE_FIRST : SQUARE_FIRST + 1, :])
        inside = norm <= lead
        killed = norm <= -lead
        safe = jnp.where(norm > 0, norm, 1.0)
        middle = 0.5 * (lead + norm)
        factor = jnp.where(inside, 1.0, jnp.where(killed, 0.0, middle / safe))
        new = jnp.where(inside, lead, jnp.where(killed, 0.0, middle))
        tails = vectors[block][TAIL_LAST : TAIL_LAST + 1, :] + vectors[block + 1][TAIL_FIRST : TAIL_FIRST + 1, :]
        total = total + ((factor - 1.0) * tails + (new - lead) * vectors[block][HEAD_LAST : HEAD_LAST + 1, :])
        tail_last = jnp.where(row == block, factor, tail_last)
        lead_last = jnp.where(row == block, new, lead_last)
        tail_first = jnp.where(row == block + 1, factor, tail_first)
    next_ref[...] = (own_lanes(blend_ref[...]) - scale_back * total)[:, 0:local]
    final = own_rows - 1
    begin, end = edge_ref[0:1, :], edge_ref[1:2, :]
    ahead = jnp.where(aux_ref[FIRST, 0:1, :] > 0, tail_first * begin, proj_ref[0:1, :])
    closing = jnp.where(aux_ref[HEAD, final : final + 1, :] > 0, lead_last, tail_last * end)
    closing = jnp.where(aux_ref[LAST, final : final + 1, :] > 0, closing, proj_ref[final : final + 1, :])
    sub = lax.broadcasted_iota(jnp.int32, (own_rows, LANES), 0)
    out_ref[...] = jnp.where(sub == 0, ahead, jnp.where(sub == final, closing, proj_ref[...]))


def exchange(x, axis, turns):
    count = lax.axis_size(axis)
    return [lax.ppermute(x, axis, [(i, i ^ turn) for i in range(count)]) for turn in turns]


def exchange_rows(x):
    rows, cols = lax.axis_size("row"), lax.axis_size("col")
    return [
        lax.ppermute(x, ("row", "col"), [(r * cols + c, (r ^ turn) * cols + (c ^ 1)) for r in range(rows) for c in range(cols)])
        for turn in range(1, rows)
    ]


def merge_kernel(own_ref, far_ref, near_ref, out_ref):
    fetched = lax.bitwise_and(lax.axis_index("col"), 1) == 1
    out_ref[...] = near_ref[...] + jnp.where(fetched, far_ref[...], own_ref[...])


def reduce_chips(x, count):
    terms, bit = [x], 2
    while bit < count:
        x = tree(terms)
        if 2 * bit < count:
            far = lax.ppermute(x, "col", [(i, i ^ (3 * bit if i % 2 else bit)) for i in range(count)])
            near = lax.ppermute(x, "col", [(i, i ^ (2 * bit if i % 2 else bit)) for i in range(count)])
            x = pl.pallas_call(
                merge_kernel,
                name="merge",
                in_specs=[vmem()] * 3,
                out_specs=vmem(),
                out_shape=jax.ShapeDtypeStruct(x.shape, F32),
                compiler_params=params(),
            )(x, far, near)
            terms = [x, *exchange(x, "col", [1])]
        else:
            terms = [x, *exchange(x, "col", [bit])]
        bit *= 4
    return terms


def body(iterates, residuals, operator, target, cone_id):
    row_count = lax.axis_size("row")
    col_count = lax.axis_size("col")
    row_block, width = operator.shape
    hist, local = iterates.shape[0] - 1, iterates.shape[1]
    all_rows = row_block * row_count
    scale_back = math.sqrt(local * row_count * col_count / all_rows)
    wide, _, rows = dims(hist, local)
    own_rows = row_block // LANES

    (other,) = exchange(operator, "col", [1])
    token = pl.pallas_call(
        token_kernel,
        name="token",
        out_specs=vmem(),
        out_shape=jax.ShapeDtypeStruct((TILE, LANES), F32),
        cost_estimate=pl.CostEstimate(flops=10**10, bytes_accessed=4 * 10**7, transcendentals=0),
        compiler_params=params(),
    )()
    message = pl.pallas_call(
        functools.partial(pack_kernel, hist, local),
        name="pack",
        in_specs=[vmem()] * 3,
        out_specs=vmem(),
        out_shape=jax.ShapeDtypeStruct((row_count * col_count * rows, LANES), F32),
        scratch_shapes=[
            pltpu.VMEM((wide, LANES), F32),
            pltpu.VMEM((-(-hist // TILE) * LANES, local), F32),
        ],
        cost_estimate=pl.CostEstimate(flops=10**10, bytes_accessed=4 * 10**7, transcendentals=0),
        compiler_params=params(),
    )(token, iterates, residuals)
    received = lax.all_to_all(message, ("col", "row"), 0, 0, tiled=True)

    *halves, part, blended = pl.pallas_call(
        functools.partial(image_kernel, hist, local, row_count, min(256, row_block)),
        name="image",
        in_specs=[vmem()] * 3,
        out_specs=[vmem()] * 6,
        out_shape=[
            *[jax.ShapeDtypeStruct((row_block, width), BF16)] * 4,
            jax.ShapeDtypeStruct((own_rows, LANES), F32),
            jax.ShapeDtypeStruct((1, width), F32),
        ],
        scratch_shapes=[
            pltpu.VMEM((width // LANES, wide, LANES), F32),
            pltpu.VMEM((width // LANES, wide, LANES), F32),
            pltpu.VMEM(((hist + 1) * own_rows, LANES), F32),
        ],
        compiler_params=params(8 * operator.size),
    )(received, operator, other)

    aux = pl.pallas_call(
        functools.partial(mask_kernel, row_count),
        name="masks",
        in_specs=[vmem()] * 3,
        out_specs=vmem(),
        out_shape=jax.ShapeDtypeStruct((AUX, own_rows, LANES), F32),
        compiler_params=params(),
    )(cone_id.reshape(-1, LANES), target.reshape(-1, LANES), blended)

    parts = reduce_chips(part, col_count)
    projected, edge, left, scalars, other = pl.pallas_call(
        functools.partial(cone_kernel, len(parts)),
        name="cones",
        in_specs=[vmem()] * (len(parts) + 3),
        out_specs=[vmem()] * 5,
        out_shape=[
            jax.ShapeDtypeStruct((own_rows, LANES), F32),
            jax.ShapeDtypeStruct((TILE, LANES), F32),
            jax.ShapeDtypeStruct((4 * TILE, row_block), BF16),
            jax.ShapeDtypeStruct((TILE, width), F32),
            jax.ShapeDtypeStruct((TILE, width), F32),
        ],
        compiler_params=params(8 * operator.size),
    )(*parts, aux, *halves[2:])
    own = pl.pallas_call(
        own_kernel,
        name="own",
        in_specs=[vmem()] * 4,
        out_specs=vmem(),
        out_shape=jax.ShapeDtypeStruct((TILE, width), F32),
        compiler_params=params(8 * operator.size),
    )(left, *halves[:2], scalars)

    turns = [0, 1, *range(3, row_count), 2]
    messages = [own, *exchange_rows(other)]
    next_point, projected = pl.pallas_call(
        functools.partial(finish_kernel, scale_back, local, row_count, turns),
        name="finish",
        in_specs=[vmem()] * (row_count + 4),
        out_specs=[vmem()] * 2,
        out_shape=[jax.ShapeDtypeStruct((1, local), F32), jax.ShapeDtypeStruct((own_rows, LANES), F32)],
        compiler_params=params(),
    )(*[messages[turn] for turn in turns], projected, edge, aux, blended)
    return (next_point.reshape(local), projected.reshape(row_block))


def solution(mesh):
    return jax.shard_map(
        body,
        mesh=mesh,
        in_specs=(P(None, ("col", "row")), P(None, ("col", "row")), P("row", "col"), P(), P()),
        out_specs=(P(("col", "row")), P("row")),
        check_vma=False,
    )
```
